32 devices in a mesh: dp: 2 (over x), expert: 16 (over z, y, core).
Axes of the slice: x: 2, y: 2, z: 4, core: 2. Of those that a mesh axis runs over, the one named last changes fastest.
Arguments:
- queries: bfloat16 [1024, 4, 3072], P('expert', 'dp'), may hold values from -256 to 256
- key_nope: bfloat16 [1024, 4, 2048], P('expert', 'dp'), may hold values from -4 to 4
- key_rope: bfloat16 [1024, 4, 64], P('expert', 'dp'), may hold values from -4 to 4
- values: bfloat16 [1024, 4, 2048], P('expert', 'dp'), may hold values from -6 to 6
- residual: bfloat16 [1024, 4, 2048], P('expert', 'dp'), may hold values from -6 to 6
- segments: int32 [4, 1024], P('dp'), may hold values from 0 to 1, never falling along the last dimension, each value on 1 to 768 neighbouring positions
- out_proj: bfloat16 [2048, 2048], P(('dp', 'expert')), may hold values from -0.125 to 0.125
- norm_gain: bfloat16 [2048], replicated, may hold values from 0.5 to 1.5
- expert_gate: bfloat16 [16, 2048, 704], P('expert'), may hold values from -0.125 to 0.125
- expert_up: bfloat16 [16, 2048, 704], P('expert'), may hold values from -0.125 to 0.125
- expert_down: bfloat16 [16, 704, 2048], P('expert'), may hold values from -0.21875 to 0.21875
- routes: int32 [2, 16, 128, 6], P('dp', 'expert'), may hold values from 0 to 15, all different within a row; in each aligned block of 128 rows (0 to 127, 128 to 255, ..., all dimensions but the last counted through in order) at most 72 rows name the same one
- route_weights: float32 [2, 16, 128, 6], P('dp', 'expert'), may hold values from 0.1 to 0.6
Outputs:
- layer_out: bfloat16 [1024, 4, 2048], P('expert', 'dp')
The draws below stay inside these ranges and needn't reach their ends.
Inputs may be any that keep to these rules, and one draw needn't show every extreme that they name: `routes`: each row names 6 different experts; within the rows of one device no expert is named more than 72 times.
All inputs are finite; a program needn't handle non-finite values.
Results may differ from the reference program's by a relative error of at most 0.0049.
Values may be sent and summed in bfloat16 or wider, within the bound.
A program may use at most 128 MiB of HBM per device.

```python
import math
import jax
import jax.numpy as jnp
import numpy as np
from jax import lax

D = 2048
HEADS = 16
NOPE = 128
ROPE = 64
V_DIM = 128
FF_E = 704
TOP = 6
STREAMS = 2
DOCS = 2
TOK_HALF = 64
QK_DIM = 192
EXPERTS = 16
LENGTH = 1024
S_ALL = 4
TOK_DEV = 128
MOST = 72
DOC_MOST = 768
N_DP = 2
N_EXPERT = 16


def key_parts(key):
    nope_part = jnp.clip(jax.random.normal(jax.random.fold_in(key, 11), (LENGTH, S_ALL, HEADS * NOPE), jnp.float32), -4.0, 4.0)
    rope_part = jnp.clip(jax.random.normal(jax.random.fold_in(key, 12), (LENGTH, S_ALL, ROPE), jnp.float32), -4.0, 4.0)
    return (nope_part, rope_part)


def draw_key_nope(key, part):
    return key_parts(key)[0].astype(jnp.bfloat16)


def draw_key_rope(key, part):
    return key_parts(key)[1].astype(jnp.bfloat16)


def draw_queries(key, part):
    drawn = jnp.clip(jax.random.normal(jax.random.fold_in(key, 15), (LENGTH, S_ALL, HEADS * QK_DIM), jnp.float32), -6.0, 6.0)
    return drawn.astype(jnp.bfloat16)


def steps_of(key, dims, shards, smallest, largest):
    def one(axis_at, shards_of):
        heights = jax.random.uniform(jax.random.fold_in(jax.random.fold_in(key, 6), axis_at), (shards_of,), jnp.float32, smallest / len(shards), largest / len(shards))
        return jnp.repeat(jnp.exp(heights), dims[axis_at] // shards_of).reshape((-1,) + (1,) * (len(dims) - axis_at - 1))

    loudness = one(*shards[0])
    for cut in shards[1:]:
        loudness = loudness * one(*cut)
    return loudness


def profile(amount, total, bound, skew):
    portions = [(1 << 20) // math.isqrt(rank ** skew) + 1 for rank in range(2, amount + 1)]
    surplus, given = total - bound - (amount - 1), [1] * (amount - 1)
    while surplus > 0:
        movable = [i for i in range(amount - 1) if given[i] < bound]
        mass, budget = sum([portions[i] for i in movable]), surplus
        for i in movable:
            more = min(bound - given[i], max(1, budget * portions[i] // mass), surplus)
            given[i] = given[i] + more
            surplus = surplus - more
    return np.array([bound] + given)


def uneven(own_key, count, total, most, lean):
    if count == 2:
        one = jax.random.randint(own_key, (), max(1, total - most), min(most, total - 1) + 1)
        return jnp.stack([one, total - one])
    sizes = jnp.asarray(profile(count, total, most, lean), jnp.int32)
    twos = (count - 1) // 2
    giver, receiver = sizes[1:1 + 2 * twos:2], sizes[2:2 + 2 * twos:2]
    slack = jnp.minimum(giver - 1, most - receiver)
    passed = jax.random.randint(jax.random.fold_in(own_key, 1), (twos,), 0, 1 << 20) % (slack + 1)
    sizes = sizes.at[1:1 + 2 * twos:2].set(giver - passed).at[2:2 + 2 * twos:2].set(receiver + passed)
    return sizes[jax.random.permutation(jax.random.fold_in(own_key, 2), count)]


def routed_block(key, own, number, rows, count, top, most, slope):
    ranking = jax.random.permutation(key, count)
    heavy_load, usual = portions_of(count, rows * top, most, slope, True), portions_of(count, rows * top, most, slope, False)
    places = jnp.arange(count)

    def named(lengths, rotation):
        used = int((lengths > 0).sum())
        fixed = max(1, used // 4)
        passed = fixed + (places - fixed + rotation * (used - fixed)) % max(1, count - fixed)
        return jnp.zeros((count,), jnp.int32).at[ranking[jnp.where(places < fixed, places, passed)]].set(jnp.asarray(lengths, jnp.int32))

    lengths = jnp.where(number % 4 == 0, named(heavy_load, number // 4), named(usual, number - number // 4 - 1))
    mixed = jax.random.permutation(jax.random.fold_in(own, 3), count)
    source_of, receiver = mixed[0:count // 2 * 2:2], mixed[1:count // 2 * 2:2]
    margin = jnp.minimum(lengths[source_of] - 1, most - lengths[receiver]) // 2
    margin = jnp.where((source_of == ranking[0]) | (receiver == ranking[0]) | (lengths[receiver] == 0), 0, jnp.maximum(margin, 0))
    passed = jax.random.randint(jax.random.fold_in(own, 4), (count // 2,), 0, 1 << 20) % (margin + 1)
    lengths = lengths.at[source_of].add(-passed).at[receiver].add(passed)
    labels = jnp.searchsorted(jnp.cumsum(lengths), jnp.arange(rows * top), side="right").astype(jnp.int32)
    grid = labels.reshape(top, rows).T
    grid = grid[jax.random.permutation(jax.random.fold_in(own, 1), rows)]
    rotation = jax.random.randint(jax.random.fold_in(own, 2), (rows, 1), 0, top)
    return jnp.take_along_axis(grid, (jnp.arange(top)[None, :] + rotation) % top, axis=1)


def portions_of(number_of, total, most, lean, full):
    loads = [(1 << 20) // math.isqrt(standing ** lean) + 1 for standing in range(1, number_of + 1)]
    largest = most if full else min(most, max(-(-total // number_of), total * loads[0] // sum(loads)))
    least = 1 if total - largest >= number_of - 1 else 0
    counts, surplus = [largest] + [least] * (number_of - 1), total - largest - least * (number_of - 1)
    while surplus > 0:
        free = [i for i in range(1, number_of) if counts[i] < largest] or [i for i in range(1, number_of) if counts[i] < most]
        pool, left = sum([loads[i] for i in free]), surplus
        for i in free:
            extra = min(most - counts[i], max(1, left * loads[i] // pool), surplus)
            counts[i] = counts[i] + extra
            surplus = surplus - extra
    return np.array(counts)


def normal_values(own_key, extent, scale, most, shards=(), held_as=jnp.bfloat16):
    values = scale * jax.random.normal(own_key, extent, jnp.float32)
    if shards:
        values = values * steps_of(own_key, extent, shards, -0.22, 0.18)
    return jnp.clip(values, -most, most).astype(held_as)


def setup_inputs(seed: int = 0) -> dict:
    streams_of = jax.random.split(jax.random.key(seed), 14)
    queries = draw_queries(jax.random.fold_in(streams_of[13], 71), 0)
    key_nope = draw_key_nope(jax.random.fold_in(streams_of[13], 71), 0)
    key_rope = draw_key_rope(jax.random.fold_in(streams_of[13], 71), 0)
    values = normal_values(streams_of[3], (LENGTH, S_ALL, HEADS * V_DIM), 1.0, 6.0, ((0, 16), (1, 2)))
    residual = normal_values(streams_of[4], (LENGTH, S_ALL, D), 1.0, 6.0, ((0, 16), (1, 2)))
    segments = jax.vmap(lambda own: jnp.searchsorted(jnp.cumsum(uneven(own, DOCS, LENGTH, DOC_MOST, 1)), jnp.arange(LENGTH), side="right"))(jax.random.split(streams_of[5], S_ALL)).reshape((S_ALL, LENGTH)).astype(jnp.int32)
    out_proj = normal_values(streams_of[6], (HEADS * V_DIM, D), (HEADS * V_DIM) ** -0.5, 0.125, ((0, 32),))
    norm_gain = jnp.clip(1.0 + 0.1 * jax.random.normal(streams_of[7], (D,), jnp.float32), 0.5, 1.5).astype(jnp.bfloat16)
    expert_gate = normal_values(streams_of[8], (EXPERTS, D, FF_E), D ** -0.5, 0.125, ((0, 16),))
    expert_up = normal_values(streams_of[9], (EXPERTS, D, FF_E), D ** -0.5, 0.125, ((0, 16),))
    expert_down = normal_values(streams_of[10], (EXPERTS, FF_E, D), FF_E ** -0.5, 0.21875, ((0, 16),))
    routes_keys = jax.random.split(jax.random.fold_in(streams_of[11], 1), N_DP * N_EXPERT * TOK_DEV // TOK_DEV)
    routes_turns = jax.random.permutation(jax.random.fold_in(streams_of[11], 3), N_DP * N_EXPERT * TOK_DEV // TOK_DEV)
    routes = jax.vmap(lambda own, number: routed_block(jax.random.fold_in(streams_of[11], 2), own, number, TOK_DEV, EXPERTS, TOP, MOST, 1))(routes_keys, routes_turns).reshape((N_DP, N_EXPERT, TOK_DEV, TOP))
    route_weights = jnp.clip(0.1 + 0.5 * jax.random.uniform(streams_of[12], (N_DP, N_EXPERT, TOK_DEV, TOP), jnp.float32) ** steps_of(streams_of[12], (N_DP, N_EXPERT, TOK_DEV, TOP), ((0, 2), (1, 16)), -0.2, 0.2), 0.1, 0.6)
    return dict(queries=queries, key_nope=key_nope, key_rope=key_rope, values=values, residual=residual, segments=segments, out_proj=out_proj, norm_gain=norm_gain, expert_gate=expert_gate, expert_up=expert_up, expert_down=expert_down, routes=routes, route_weights=route_weights)


EPSILON = 1e-06

def to_streams(block_array):
    width = block_array.shape[-1]
    shaped = block_array.reshape(N_DP, N_EXPERT, TOK_HALF, STREAMS, width)
    shaped = jnp.transpose(shaped, (1, 2, 0, 3, 4))
    return shaped.reshape(LENGTH, S_ALL, width)

def feed_forward(rows, gate_matrix, up_matrix, down_matrix):
    gate_part = jnp.dot(rows, gate_matrix, preferred_element_type=jnp.float32)
    up_part = jnp.dot(rows, up_matrix, preferred_element_type=jnp.float32)
    activated = (jax.nn.silu(gate_part) * up_part).astype(jnp.bfloat16)
    return jnp.dot(activated, down_matrix, preferred_element_type=jnp.float32).astype(jnp.bfloat16)

def attend_stream(inputs):
    query_rows, nope_rows, rope_rows, value_rows, segment_row = inputs
    query_heads = query_rows.reshape(LENGTH, HEADS, QK_DIM).astype(jnp.float32)
    key_heads = jnp.concatenate([nope_rows.reshape(LENGTH, HEADS, NOPE), jnp.broadcast_to(rope_rows[:, None, :], (LENGTH, HEADS, ROPE))], axis=2).astype(jnp.float32)
    value_heads = value_rows.reshape(LENGTH, HEADS, V_DIM).astype(jnp.float32)
    scores = jnp.einsum('qhd,khd->hqk', query_heads, key_heads) * QK_DIM ** (-0.5)
    positions = jnp.arange(LENGTH, dtype=jnp.int32)
    allowed = (positions[:, None] >= positions[None, :]) & (segment_row[:, None] == segment_row[None, :])
    scores = jnp.where(allowed[None], scores, -jnp.inf)
    row_peak = lax.optimization_barrier(jnp.max(scores, axis=2, keepdims=True))
    raised = jnp.exp(scores - row_peak)
    probs = (raised / lax.optimization_barrier(jnp.sum(raised, axis=2, keepdims=True))).astype(jnp.bfloat16)
    mixed = jnp.einsum('hqk,khd->qhd', probs.astype(jnp.float32), value_heads)
    return mixed.reshape(LENGTH, HEADS * V_DIM).astype(jnp.bfloat16)

def reference(queries, key_nope, key_rope, values, residual, segments, out_proj, norm_gain, expert_gate, expert_up, expert_down, routes, route_weights):
    inputs = (jnp.swapaxes(queries, 0, 1), jnp.swapaxes(key_nope, 0, 1), jnp.swapaxes(key_rope, 0, 1), jnp.swapaxes(values, 0, 1), segments)
    attended = lax.map(attend_stream, inputs)
    token_count = LENGTH * S_ALL
    attn_rows = jnp.swapaxes(attended, 0, 1).reshape(token_count, HEADS * V_DIM)
    projected = jnp.dot(attn_rows, out_proj, preferred_element_type=jnp.float32)
    hidden = residual.reshape(token_count, D).astype(jnp.float32) + projected
    mean_square = lax.optimization_barrier(jnp.mean(hidden * hidden, axis=1, keepdims=True))
    normed = (hidden * lax.rsqrt(mean_square + EPSILON) * norm_gain.astype(jnp.float32)).astype(jnp.bfloat16)
    chosen = to_streams(routes).reshape(token_count, TOP)
    scales = to_streams(route_weights).reshape(token_count, TOP)
    capacity = min(N_DP * N_EXPERT * MOST, token_count)
    row_ids = jnp.arange(token_count, dtype=jnp.int32)

    def one_expert(routed_total, expert_inputs):
        gate_matrix, up_matrix, down_matrix, expert_id = expert_inputs
        matches = chosen == expert_id
        picked = jnp.any(matches, axis=1)
        weight_row = lax.optimization_barrier(jnp.sum(jnp.where(matches, scales, jnp.zeros_like(scales)), axis=1))
        live_order = (jnp.cumsum(picked.astype(jnp.int32)) - 1).astype(jnp.int32)
        live_place = jnp.where(picked, live_order, capacity).astype(jnp.int32)
        source_rows = jnp.zeros((capacity,), jnp.int32).at[live_place].set(row_ids, mode='drop')
        filled = jnp.zeros((capacity,), jnp.int32).at[live_place].set(1, mode='drop')
        outputs = feed_forward(normed[source_rows], gate_matrix, up_matrix, down_matrix)
        contribution = (filled > 0)[:, None] * weight_row[source_rows][:, None] * outputs.astype(jnp.float32)
        return (routed_total.at[source_rows].add(contribution), expert_id)
    expert_ids = jnp.arange(EXPERTS, dtype=jnp.int32)
    routed_total = lax.scan(one_expert, jnp.zeros((token_count, D), jnp.float32), (expert_gate, expert_up, expert_down, expert_ids))[0]
    layer_out = (hidden + routed_total).astype(jnp.bfloat16)
    return layer_out.reshape(LENGTH, S_ALL, D)
```

```python
import functools

import jax
import jax.numpy as jnp
from jax import lax
from jax.experimental import pallas as pl
from jax.experimental.pallas import tpu as pltpu
from jax.sharding import PartitionSpec as P

HEADS = 16
NOPE = 128
ROPE = 64
V_DIM = 128
TOP = 6


EPSILON = 1e-06
QUERY_BLOCK = 512


MESH = pl.DeviceIdType.MESH


def ring_position(chip, chips):
    odd = chip % 2
    return (1 - odd) * (chip // 2) + odd * (chips - 1 - chip // 2)


def ring_chip(position, chips):
    back = position // (chips // 2)
    return (1 - back) * (2 * position) + back * (2 * (chips - 1 - position) + 1)


def expert_kernel(
    chips,
    x_ref,
    table_ref,
    hidden_ref,
    gate_ref,
    up_ref,
    down_ref,
    out_ref,
    rows_all,
    table_all,
    own_part,
    mate_part,
    ring_in,
    act,
    gate_vmem,
    up_vmem,
    down_vmem,
    weight_sem,
    x_send,
    x_recv,
    t_send,
    t_recv,
    m_send,
    m_recv,
    r_send,
    r_recv,
):
    tokens, width = x_ref.shape
    half = tokens // 2
    far = chips // 2
    me = lax.axis_index("expert")
    core = me % 2
    position = ring_position(me // 2, chips)
    after = 2 * ring_chip((position + 1) % chips, chips) + core
    before = 2 * ring_chip((position + chips - 1) % chips, chips) + core
    mate = me + 1 - 2 * core
    def slot_of(way, distance):
        if distance == 0:
            return 0
        if distance == far:
            return chips - 1
        return 2 * distance - 1 + way

    def reach(way, part):
        return far if part == way else far - 1

    targets = (after, before)

    barrier = pltpu.get_barrier_semaphore()
    for other in (after, before, mate):
        pl.semaphore_signal(barrier, inc=1, device_id={"expert": other}, device_id_type=MESH)

    loads = [
        pltpu.make_async_copy(src, dst, weight_sem.at[i])
        for i, (src, dst) in enumerate(
            ((gate_ref, gate_vmem), (up_ref, up_vmem), (down_ref, down_vmem))
        )
    ]
    for load in loads:
        load.start()
    pl.semaphore_wait(barrier, 3)

    def remote(src, dst, send, recv, other):
        return pltpu.make_async_remote_copy(
            src_ref=src,
            dst_ref=dst,
            send_sem=send,
            recv_sem=recv,
            device_id={"expert": other},
            device_id_type=MESH,
        )

    def rows_of(part):
        return pl.ds(part * half, half)

    def row_copy(way, distance, part):
        if way == 2:
            slot = distance
            src = x_ref.at[rows_of(part)] if slot == 0 else rows_all.at[slot, 0, rows_of(part)]
            dst = rows_all.at[slot, 1, rows_of(part)]
            other = mate
        else:
            slot = slot_of(way, distance)
            src = (
                x_ref.at[rows_of(part)]
                if distance == 1
                else rows_all.at[slot_of(way, distance - 1), 0, rows_of(part)]
            )
            dst = rows_all.at[slot, 0, rows_of(part)]
            other = targets[way]
        return remote(
            src, dst, x_send.at[way, distance, part], x_recv.at[way, distance, part], other
        )

    def table_copy(way, distance):
        if way == 2:
            slot = distance
            src = table_ref if slot == 0 else table_all.at[slot, 0]
            dst = table_all.at[slot, 1]
            other = mate
        else:
            slot = slot_of(way, distance)
            src = table_ref if distance == 1 else table_all.at[slot_of(way, distance - 1), 0]
            dst = table_all.at[slot, 0]
            other = targets[way]
        return remote(src, dst, t_send.at[way, distance], t_recv.at[way, distance], other)

    sent = []

    def start(copy):
        copy.start()
        sent.append(copy)

    def table_goes(way, distance):
        return distance < far or way == 0

    for part in range(2):
        for way in range(2):
            start(row_copy(way, 1, (part + way) % 2))
        start(row_copy(2, 0, part))
    for way in range(2):
        start(table_copy(way, 1))
    start(table_copy(2, 0))

    def serve(distance, turn):
        for way in range(2):
            part = (turn + way) % 2
            if distance > reach(way, part):
                continue
            row_copy(way, distance, part).wait_recv()
            if distance + 1 <= reach(way, part):
                start(row_copy(way, distance + 1, part))
            start(row_copy(2, slot_of(way, distance), part))
            if turn == 0 and table_goes(way, distance):
                table_copy(way, distance).wait_recv()
                if distance + 1 <= far and table_goes(way, distance + 1):
                    start(table_copy(way, distance + 1))
                start(table_copy(2, slot_of(way, distance)))

    def mate_copy(slot):
        return remote(
            rows_all.at[slot, 1], mate_part.at[slot], m_send.at[slot], m_recv.at[slot], mate
        )

    hidden_units = gate_vmem.shape[0]
    eye = lax.broadcasted_iota(jnp.int32, (tokens, tokens), 0) == lax.broadcasted_iota(
        jnp.int32, (tokens, tokens), 1
    )

    def column(row):
        return jnp.sum(jnp.where(eye, row, 0.0), axis=1, keepdims=True)

    def experts(slot):
        for part in range(2):
            row_copy(2, slot, part).wait_recv()
        table_copy(2, slot).wait_recv()
        mine = x_ref[...] if slot == 0 else rows_all[slot, 0]
        rows = jnp.concatenate([mine, rows_all[slot, 1]], axis=0)
        for first in range(0, hidden_units, 256):
            count = min(256, hidden_units - first)
            dims = (((1,), (1,)), ((), ()))
            gate_part = lax.dot_general(
                rows, gate_vmem[first : first + count, :], dims, preferred_element_type=jnp.float32
            )
            up_part = lax.dot_general(
                rows, up_vmem[first : first + count, :], dims, preferred_element_type=jnp.float32
            )
            silu = gate_part / (1.0 + jnp.exp(-gate_part))
            act[:, first : first + count] = (silu * up_part).astype(jnp.bfloat16)
        own_table = table_ref if slot == 0 else table_all.at[slot, 0]
        own_column = column(own_table[pl.ds(me, 1), :])
        mate_column = column(table_all[slot, 1, pl.ds(me, 1), :])
        for first in range(0, width, 512):
            y = jnp.dot(
                act[...], down_vmem[:, first : first + 512], preferred_element_type=jnp.float32
            )
            own_part[slot, :, first : first + 512] = (y[:tokens] * own_column).astype(jnp.bfloat16)
            rows_all[slot, 1, :, first : first + 512] = (y[tokens:] * mate_column).astype(
                jnp.bfloat16
            )
        start(mate_copy(slot))

    def sum_slot(way, distance):
        return slot_of(1 - way, distance)

    def sum_copy(way, distance, part):
        return remote(
            own_part.at[sum_slot(way, distance), rows_of(part)],
            ring_in.at[way, distance - 1, part],
            r_send.at[way, distance, part],
            r_recv.at[way, distance, part],
            targets[way],
        )

    mated = set()

    def mated_wait(slot):
        if slot not in mated:
            mated.add(slot)
            mate_copy(slot).wait_recv()

    def chip_sum(slot, part):
        mated_wait(slot)
        return own_part[slot, rows_of(part), :].astype(jnp.float32) + mate_part[
            slot, rows_of(part), :
        ].astype(jnp.float32)

    def send_sum(distance, late):
        for way in range(2):
            part = way if late else 1 - way
            if distance > reach(way, part):
                continue
            slot = sum_slot(way, distance)
            total = chip_sum(slot, part)
            if distance < reach(way, part):
                sum_copy(way, distance + 1, part).wait_recv()
                total = total + ring_in[way, distance, part].astype(jnp.float32)
            own_part[slot, rows_of(part), :] = total.astype(jnp.bfloat16)
            start(sum_copy(way, distance, part))

    for load in loads:
        load.wait()
    experts(0)
    serve(1, 0)
    serve(1, 1)
    for distance in range(1, far):
        experts(slot_of(0, distance))
        serve(distance + 1, 0)
        experts(slot_of(1, distance))
        if distance + 1 < far:
            serve(distance + 1, 1)
    send_sum(far - 1, False)
    experts(slot_of(0, far))
    send_sum(far, True)
    for distance in range(far - 2, 0, -1):
        send_sum(distance, False)
        send_sum(distance + 1, True)
    send_sum(1, True)
    for part in range(2):
        total = hidden_ref[rows_of(part), :] + chip_sum(0, part)
        for way in range(2):
            sum_copy(way, 1, part).wait_recv()
            total = total + ring_in[way, 0, part].astype(jnp.float32)
        out_ref[rows_of(part), :] = total.astype(jnp.bfloat16)
    for copy in sent:
        copy.wait_send()


def routed_experts(normed, table, hidden, gate, up, down):
    tokens, width = normed.shape
    count = table.shape[0]
    chips = count // 2
    units = gate.shape[0]
    half = tokens // 2
    vmem = pl.BlockSpec(memory_space=pltpu.VMEM)
    anywhere = pl.BlockSpec(memory_space=pl.ANY)
    dma = pltpu.SemaphoreType.DMA
    far = chips // 2
    return pl.pallas_call(
        functools.partial(expert_kernel, chips),
        out_shape=jax.ShapeDtypeStruct((tokens, width), jnp.bfloat16),
        in_specs=[vmem, vmem, vmem, anywhere, anywhere, anywhere],
        out_specs=vmem,
        scratch_shapes=[
            pltpu.VMEM((chips, 2, tokens, width), jnp.bfloat16),
            pltpu.VMEM((chips, 2, count, tokens), jnp.float32),
            pltpu.VMEM((chips, tokens, width), jnp.bfloat16),
            pltpu.VMEM((chips, tokens, width), jnp.bfloat16),
            pltpu.VMEM((2, far, 2, half, width), jnp.bfloat16),
            pltpu.VMEM((2 * tokens, units), jnp.bfloat16),
            pltpu.VMEM((units, width), jnp.bfloat16),
            pltpu.VMEM((units, width), jnp.bfloat16),
            pltpu.VMEM((units, width), jnp.bfloat16),
            dma((3,)),
            dma((3, chips, 2)),
            dma((3, chips, 2)),
            dma((3, chips)),
            dma((3, chips)),
            dma((chips,)),
            dma((chips,)),
            dma((2, far + 1, 2)),
            dma((2, far + 1, 2)),
        ],
        compiler_params=pltpu.CompilerParams(
            collective_id=1, has_side_effects=True, vmem_limit_bytes=64000000
        ),
    )(normed, table, hidden, gate, up, down)


def attend_items(query_items, key_items, value_items, segment_items):
    length, count_items, qk_width = query_items.shape
    block_rows = QUERY_BLOCK
    score_scale = qk_width ** (-0.5)
    key_positions = jnp.arange(length, dtype=jnp.int32)

    def one_block(block_index):
        first_row = block_index * block_rows
        query_block = lax.dynamic_slice_in_dim(query_items, first_row, block_rows, 0)
        scores = (
            jnp.einsum("qid,kid->iqk", query_block, key_items, preferred_element_type=jnp.float32)
            * score_scale
        )
        row_positions = first_row + jnp.arange(block_rows, dtype=jnp.int32)
        row_segments = lax.dynamic_slice_in_dim(segment_items, first_row, block_rows, 1)
        allowed = (row_positions[None, :, None] >= key_positions[None, None, :]) & (
            row_segments[:, :, None] == segment_items[:, None, :]
        )
        scores = jnp.where(allowed, scores, -jnp.inf)
        row_peak = jnp.max(scores, axis=2, keepdims=True)
        raised = jnp.exp(scores - row_peak)
        weights = (raised / jnp.sum(raised, axis=2, keepdims=True)).astype(jnp.bfloat16)
        return jnp.einsum(
            "iqk,kid->qid", weights, value_items, preferred_element_type=jnp.float32
        ).astype(jnp.bfloat16)

    blocks = lax.map(one_block, jnp.arange(length // block_rows, dtype=jnp.int32))
    return blocks.reshape(length, count_items, value_items.shape[2])


def body(
    queries,
    key_nope,
    key_rope,
    values,
    residual,
    segments,
    out_proj,
    norm_gain,
    expert_gate,
    expert_up,
    expert_down,
    routes,
    route_weights,
):
    half_rows, stream_count, query_width = queries.shape
    model_width = residual.shape[2]
    token_rows = half_rows * stream_count
    expert_count = lax.axis_size("expert")
    item_count = stream_count * HEADS // expert_count
    key_heads = jnp.concatenate(
        [
            key_nope.reshape(half_rows, stream_count, HEADS, NOPE),
            jnp.broadcast_to(key_rope[:, :, None, :], (half_rows, stream_count, HEADS, ROPE)),
        ],
        axis=3,
    )
    query_items = queries.reshape(half_rows, stream_count * HEADS, NOPE + ROPE)
    key_items = key_heads.reshape(half_rows, stream_count * HEADS, NOPE + ROPE)
    value_items = values.reshape(half_rows, stream_count * HEADS, V_DIM)
    packed = jnp.concatenate([query_items, key_items, value_items], axis=2)
    packed_all = lax.all_to_all(packed, "expert", split_axis=1, concat_axis=0, tiled=True)
    qk_width = NOPE + ROPE
    query_all = packed_all[:, :, :qk_width]
    key_all = packed_all[:, :, qk_width : 2 * qk_width]
    value_all = packed_all[:, :, 2 * qk_width :]
    item_ids = lax.axis_index("expert") * item_count + jnp.arange(item_count, dtype=jnp.int32)
    stream_ids = item_ids // HEADS
    selector = (stream_ids[:, None] == jnp.arange(stream_count, dtype=jnp.int32)[None, :]).astype(
        jnp.int32
    )
    segment_items = jnp.sum(selector[:, :, None] * segments[None, :, :], axis=1)
    attended_items = attend_items(query_all, key_all, value_all, segment_items)
    attended_back = lax.all_to_all(
        attended_items, "expert", split_axis=0, concat_axis=1, tiled=True
    )
    attn_rows = attended_back.reshape(token_rows, HEADS * V_DIM)
    projected = jnp.dot(
        attn_rows,
        lax.all_gather(out_proj, ("dp", "expert"), axis=0, tiled=True),
        preferred_element_type=jnp.float32,
    )
    hidden = residual.reshape(token_rows, model_width).astype(jnp.float32) + projected
    mean_square = jnp.mean(hidden * hidden, axis=1, keepdims=True)
    normed = (hidden * lax.rsqrt(mean_square + EPSILON) * norm_gain.astype(jnp.float32)).astype(
        jnp.bfloat16
    )
    token_routes = routes.reshape(token_rows, TOP)
    token_weights = route_weights.reshape(token_rows, TOP)
    expert_ids = jnp.arange(expert_count, dtype=jnp.int32)
    weight_table = jnp.sum(
        jnp.where(
            token_routes[:, :, None] == expert_ids[None, None, :], token_weights[:, :, None], 0.0
        ),
        axis=1,
    )
    layer_out = routed_experts(
        normed,
        weight_table.T,
        hidden,
        jnp.swapaxes(expert_gate[0], 0, 1),
        jnp.swapaxes(expert_up[0], 0, 1),
        expert_down[0],
    )
    return layer_out.reshape(half_rows, stream_count, model_width)


def solution(mesh):
    return jax.shard_map(
        body,
        mesh=mesh,
        in_specs=(
            P("expert", "dp", None),
            P("expert", "dp", None),
            P("expert", "dp", None),
            P("expert", "dp", None),
            P("expert", "dp", None),
            P("dp", None),
            P(("dp", "expert"), None),
            P(),
            P("expert", None, None),
            P("expert", None, None),
            P("expert", None, None),
            P("dp", "expert", None, None),
            P("dp", "expert", None, None),
        ),
        out_specs=P("expert", "dp", None),
        check_vma=False,
    )
```

```python
import functools

import jax
import jax.numpy as jnp
from jax import lax
from jax.experimental import pallas as pl
from jax.experimental.pallas import tpu as pltpu
from jax.sharding import PartitionSpec as P

HEADS = 16
NOPE = 128
ROPE = 64
V_DIM = 128
TOP = 6


EPSILON = 1e-06
QUERY_BLOCK = 512


MESH = pl.DeviceIdType.MESH


def ring_position(chip, chips):
    odd = chip % 2
    return (1 - odd) * (chip // 2) + odd * (chips - 1 - chip // 2)


def ring_chip(position, chips):
    back = position // (chips // 2)
    return (1 - back) * (2 * position) + back * (2 * (chips - 1 - position) + 1)


def expert_kernel(
    chips,
    x_ref,
    table_ref,
    hidden_ref,
    gate_ref,
    up_ref,
    down_ref,
    out_ref,
    rows_all,
    table_all,
    own_part,
    mate_part,
    ring_in,
    act,
    gate_vmem,
    up_vmem,
    down_vmem,
    weight_sem,
    x_send,
    x_recv,
    t_send,
    t_recv,
    m_send,
    m_recv,
    r_send,
    r_recv,
):
    tokens, width = x_ref.shape
    half = tokens // 2
    far = chips // 2
    me = lax.axis_index("expert")
    core = me % 2
    position = ring_position(me // 2, chips)
    after = 2 * ring_chip((position + 1) % chips, chips) + core
    before = 2 * ring_chip((position + chips - 1) % chips, chips) + core
    mate = me + 1 - 2 * core
    def slot_of(way, distance):
        if distance == 0:
            return 0
        if distance == far:
            return chips - 1
        return 2 * distance - 1 + way

    def reach(way, part):
        return far if part == way else far - 1

    targets = (after, before)

    barrier = pltpu.get_barrier_semaphore()
    for other in (after, before, mate):
        pl.semaphore_signal(barrier, inc=1, device_id={"expert": other}, device_id_type=MESH)

    loads = [
        pltpu.make_async_copy(src, dst, weight_sem.at[i])
        for i, (src, dst) in enumerate(
            ((gate_ref, gate_vmem), (up_ref, up_vmem), (down_ref, down_vmem))
        )
    ]
    for load in loads:
        load.start()
    pl.semaphore_wait(barrier, 3)

    def remote(src, dst, send, recv, other):
        return pltpu.make_async_remote_copy(
            src_ref=src,
            dst_ref=dst,
            send_sem=send,
            recv_sem=recv,
            device_id={"expert": other},
            device_id_type=MESH,
        )

    def rows_of(part):
        return pl.ds(part * half, half)

    def row_copy(way, distance, part):
        if way == 2:
            slot = distance
            src = x_ref.at[rows_of(part)] if slot == 0 else rows_all.at[slot, 0, rows_of(part)]
            dst = rows_all.at[slot, 1, rows_of(part)]
            other = mate
        else:
            slot = slot_of(way, distance)
            src = (
                x_ref.at[rows_of(part)]
                if distance == 1
                else rows_all.at[slot_of(way, distance - 1), 0, rows_of(part)]
            )
            dst = rows_all.at[slot, 0, rows_of(part)]
            other = targets[way]
        return remote(
            src, dst, x_send.at[way, distance, part], x_recv.at[way, distance, part], other
        )

    def table_copy(way, distance):
        if way == 2:
            slot = distance
            src = table_ref if slot == 0 else table_all.at[slot, 0]
            dst = table_all.at[slot, 1]
            other = mate
        else:
            slot = slot_of(way, distance)
            src = table_ref if distance == 1 else table_all.at[slot_of(way, distance - 1), 0]
            dst = table_all.at[slot, 0]
            other = targets[way]
        return remote(src, dst, t_send.at[way, distance], t_recv.at[way, distance], other)

    sent = []

    def start(copy):
        copy.start()
        sent.append(copy)

    def table_goes(way, distance):
        return distance < far or way == 0

    for part in range(2):
        for way in range(2):
            start(row_copy(way, 1, (part + way) % 2))
        start(row_copy(2, 0, part))
    for way in range(2):
        start(table_copy(way, 1))
    start(table_copy(2, 0))

    def serve(distance, turn):
        for way in range(2):
            part = (turn + way) % 2
            if distance > reach(way, part):
                continue
            row_copy(way, distance, part).wait_recv()
            if distance + 1 <= reach(way, part):
                start(row_copy(way, distance + 1, part))
            start(row_copy(2, slot_of(way, distance), part))
            if turn == 0 and table_goes(way, distance):
                table_copy(way, distance).wait_recv()
                if distance + 1 <= far and table_goes(way, distance + 1):
                    start(table_copy(way, distance + 1))
                start(table_copy(2, slot_of(way, distance)))

    def mate_copy(slot):
        return remote(
            rows_all.at[slot, 1], mate_part.at[slot], m_send.at[slot], m_recv.at[slot], mate
        )

    hidden_units = gate_vmem.shape[0]
    eye = lax.broadcasted_iota(jnp.int32, (tokens, tokens), 0) == lax.broadcasted_iota(
        jnp.int32, (tokens, tokens), 1
    )

    def column(row):
        return jnp.sum(jnp.where(eye, row, 0.0), axis=1, keepdims=True)

    def experts(slot):
        for part in range(2):
            row_copy(2, slot, part).wait_recv()
        table_copy(2, slot).wait_recv()
        mine = x_ref[...] if slot == 0 else rows_all[slot, 0]
        rows = jnp.concatenate([mine, rows_all[slot, 1]], axis=0)
        for first in range(0, hidden_units, 256):
            count = min(256, hidden_units - first)
            dims = (((1,), (1,)), ((), ()))
            gate_part = lax.dot_general(
                rows, gate_vmem[first : first + count, :], dims, preferred_element_type=jnp.float32
            )
            up_part = lax.dot_general(
                rows, up_vmem[first : first + count, :], dims, preferred_element_type=jnp.float32
            )
            silu = gate_part / (1.0 + jnp.exp(-gate_part))
            act[:, first : first + count] = (silu * up_part).astype(jnp.bfloat16)
        own_table = table_ref if slot == 0 else table_all.at[slot, 0]
        own_column = column(own_table[pl.ds(me, 1), :])
        mate_column = column(table_all[slot, 1, pl.ds(me, 1), :])
        for first in range(0, width, 512):
            y = jnp.dot(
                act[...], down_vmem[:, first : first + 512], preferred_element_type=jnp.float32
            )
            own_part[slot, :, first : first + 512] = (y[:tokens] * own_column).astype(jnp.bfloat16)
            rows_all[slot, 1, :, first : first + 512] = (y[tokens:] * mate_column).astype(
                jnp.bfloat16
            )
        start(mate_copy(slot))

    def sum_slot(way, distance):
        return slot_of(1 - way, distance)

    def sum_copy(way, distance, part):
        return remote(
            own_part.at[sum_slot(way, distance), rows_of(part)],
            ring_in.at[way, distance - 1, part],
            r_send.at[way, distance, part],
            r_recv.at[way, distance, part],
            targets[way],
        )

    mated = set()

    def mated_wait(slot):
        if slot not in mated:
            mated.add(slot)
            mate_copy(slot).wait_recv()

    def chip_sum(slot, part):
        mated_wait(slot)
        return own_part[slot, rows_of(part), :].astype(jnp.float32) + mate_part[
            slot, rows_of(part), :
        ].astype(jnp.float32)

    def send_sum(distance, late):
        for way in range(2):
            part = way if late else 1 - way
            if distance > reach(way, part):
                continue
            slot = sum_slot(way, distance)
            total = chip_sum(slot, part)
            if distance < reach(way, part):
                sum_copy(way, distance + 1, part).wait_recv()
                total = total + ring_in[way, distance, part].astype(jnp.float32)
            own_part[slot, rows_of(part), :] = total.astype(jnp.bfloat16)
            start(sum_copy(way, distance, part))

    for load in loads:
        load.wait()
    experts(0)
    serve(1, 0)
    serve(1, 1)
    for distance in range(1, far):
        experts(slot_of(0, distance))
        serve(distance + 1, 0)
        experts(slot_of(1, distance))
        if distance + 1 < far:
            serve(distance + 1, 1)
    send_sum(far - 1, False)
    experts(slot_of(0, far))
    send_sum(far, True)
    for distance in range(far - 2, 0, -1):
        send_sum(distance, False)
        send_sum(distance + 1, True)
    send_sum(1, True)
    for part in range(2):
        total = hidden_ref[rows_of(part), :] + chip_sum(0, part)
        for way in range(2):
            sum_copy(way, 1, part).wait_recv()
            total = total + ring_in[way, 0, part].astype(jnp.float32)
        out_ref[rows_of(part), :] = total.astype(jnp.bfloat16)
    for copy in sent:
        copy.wait_send()


def routed_experts(normed, table, hidden, gate, up, down):
    tokens, width = normed.shape
    count = table.shape[0]
    chips = count // 2
    units = gate.shape[0]
    half = tokens // 2
    vmem = pl.BlockSpec(memory_space=pltpu.VMEM)
    anywhere = pl.BlockSpec(memory_space=pl.ANY)
    dma = pltpu.SemaphoreType.DMA
    far = chips // 2
    return pl.pallas_call(
        functools.partial(expert_kernel, chips),
        out_shape=jax.ShapeDtypeStruct((tokens, width), jnp.bfloat16),
        in_specs=[vmem, vmem, vmem, anywhere, anywhere, anywhere],
        out_specs=vmem,
        scratch_shapes=[
            pltpu.VMEM((chips, 2, tokens, width), jnp.bfloat16),
            pltpu.VMEM((chips, 2, count, tokens), jnp.float32),
            pltpu.VMEM((chips, tokens, width), jnp.bfloat16),
            pltpu.VMEM((chips, tokens, width), jnp.bfloat16),
            pltpu.VMEM((2, far, 2, half, width), jnp.bfloat16),
            pltpu.VMEM((2 * tokens, units), jnp.bfloat16),
            pltpu.VMEM((units, width), jnp.bfloat16),
            pltpu.VMEM((units, width), jnp.bfloat16),
            pltpu.VMEM((units, width), jnp.bfloat16),
            dma((3,)),
            dma((3, chips, 2)),
            dma((3, chips, 2)),
            dma((3, chips)),
            dma((3, chips)),
            dma((chips,)),
            dma((chips,)),
            dma((2, far + 1, 2)),
            dma((2, far + 1, 2)),
        ],
        compiler_params=pltpu.CompilerParams(
            collective_id=1, has_side_effects=True, vmem_limit_bytes=64000000
        ),
    )(normed, table, hidden, gate, up, down)


def flip(device, bit):
    return device + bit - 2 * bit * ((device // bit) % 2)


def attention_kernel(
    peers,
    q_ref,
    nope_ref,
    rope_ref,
    value_ref,
    residual_ref,
    segments_ref,
    proj_ref,
    gain_ref,
    hidden_ref,
    normed_ref,
    q_own,
    q_stage,
    mix_stage,
    q_in,
    mix_in,
    nope_in,
    value_in,
    q_all,
    key_all,
    value_all,
    out_stage,
    attn,
    proj,
    load_sem,
    a_send,
    a_recv,
    b_send,
    b_recv,
    c_send,
    c_recv,
):
    block, streams, _ = q_ref.shape
    length = block * peers
    head = NOPE
    width = proj_ref.shape[1]
    proj_rows = proj_ref.shape[0]
    me = lax.axis_index("expert")
    plane = lax.axis_index("dp")
    mate, row_mate = flip(me, 1), flip(me, 2)
    near, far = flip(me, peers // 4), flip(me, peers // 2)

    barrier = pltpu.get_barrier_semaphore()
    for offset in range(1, peers):
        pl.semaphore_signal(
            barrier,
            inc=1,
            device_id={"dp": plane, "expert": (me + offset) % peers},
            device_id_type=MESH,
        )
    pl.semaphore_signal(
        barrier, inc=1, device_id={"dp": 1 - plane, "expert": me}, device_id_type=MESH
    )

    def own_columns(first):
        return pl.ds(pl.multiple_of(first, head), head)

    def own_places(device):
        return pl.ds(pl.multiple_of(device * block, block), block)

    def proj_place(part, device):
        return pl.ds(
            pl.multiple_of((part * peers + device) * proj_rows, proj_rows), proj_rows
        )

    load_q = pltpu.make_async_copy(q_ref, q_own, load_sem.at[0])
    load_rope = pltpu.make_async_copy(rope_ref, mix_stage.at[0], load_sem.at[1])
    load_proj = pltpu.make_async_copy(
        proj_ref, proj.at[proj_place(plane, me)], load_sem.at[2]
    )
    for load in (load_q, load_rope, load_proj):
        load.start()
    pl.semaphore_wait(barrier, peers)

    def remote(src, dst, send, recv, part, other):
        return pltpu.make_async_remote_copy(
            src_ref=src,
            dst_ref=dst,
            send_sem=send,
            recv_sem=recv,
            device_id={"dp": part, "expert": other},
            device_id_type=MESH,
        )

    sent = []

    def start(copy):
        copy.start()
        sent.append(copy)

    partners = (
        (plane, far),
        (plane, near),
        (plane, row_mate),
        (1 - plane, me),
        (plane, mate),
    )

    def proj_copy(stage, index, src_part, src_device, from_input=False):
        place = proj.at[proj_place(src_part, src_device)]
        part, other = partners[stage]
        return remote(
            proj_ref if from_input else place,
            place,
            c_send.at[stage, index],
            c_recv.at[stage, index],
            part,
            other,
        )

    def proj_source(index, of_device, of_part):
        device = of_device
        if index & 1:
            device = flip(device, peers // 2)
        if index & 2:
            device = flip(device, peers // 4)
        if index & 4:
            device = flip(device, 2)
        return (1 - of_part if index & 8 else of_part), device

    def proj_forward(index):
        first = index.bit_length()
        part, device = proj_source(index, me, plane)
        for stage in range(first, 5):
            start(proj_copy(stage, index, part, device, from_input=index == 0))

    def proj_wait(index):
        stage = index.bit_length() - 1
        part, device = proj_source(index, me, plane)
        proj_copy(stage, index - (1 << stage), part, device).wait_recv()

    def proj_serve(index):
        proj_wait(index)
        proj_forward(index)

    proj_forward(0)

    def block_copies(target, source_places):
        return (
            (q_stage.at[target], q_in.at[source_places]),
            (mix_stage.at[target + 1], mix_in.at[source_places]),
            (nope_ref.at[:, :, own_columns(target * head)], nope_in.at[source_places]),
            (value_ref.at[:, :, own_columns(target * head)], value_in.at[source_places]),
        )

    def a_copy(offset, which):
        target = (me + offset) % peers
        src, dst = block_copies(target, own_places(me))[which]
        return remote(
            src, dst, a_send.at[offset, which], a_recv.at[offset, which], plane, target
        )

    order = sorted(range(1, peers), key=lambda offset: (abs(offset - peers // 2), offset))
    for offset in order[:3]:
        for which in (2, 3):
            start(a_copy(offset, which))

    load_q.wait()
    load_rope.wait()
    lane = lax.broadcasted_iota(jnp.int32, (block * streams, head), 1)
    low = lane < ROPE

    def wide(x):
        return x.astype(jnp.float32)

    def turn(x):
        return pltpu.roll(x, ROPE, 1)

    rope_low = wide(mix_stage[0].reshape(block * streams, head))
    rope_high = turn(rope_low)
    for pair in range(HEADS // 2):
        first = pair * 3 * head
        one, two, three = (
            q_own[:, :, first + i * head : first + (i + 1) * head].reshape(block * streams, head)
            for i in range(3)
        )
        two, three = wide(two), wide(three)
        shape = (block, streams, head)

        def narrow(x):
            return x.astype(jnp.bfloat16).reshape(shape)

        q_stage[2 * pair] = one.reshape(shape)
        mix_stage[2 * pair + 1] = narrow(jnp.where(low, two, rope_high))
        q_stage[2 * pair + 1] = narrow(turn(jnp.where(low, three, two)))
        mix_stage[2 * pair + 2] = narrow(jnp.where(low, rope_low, three))
    for offset in order[:3]:
        for which in (0, 1):
            start(a_copy(offset, which))
    own = [
        pltpu.make_async_copy(src, dst, load_sem.at[3 + i])
        for i, (src, dst) in enumerate(block_copies(me, own_places(me)))
    ]
    for copy in own:
        copy.start()
    proj_serve(1)
    for offset in order[3:]:
        for which in range(4):
            start(a_copy(offset, which))

    odd = jnp.full((block, head), me % 2, jnp.int32)
    here = lax.broadcasted_iota(jnp.int32, (block, head), 1) // ROPE
    kept = here == odd

    def unpack(device):
        places = own_places(device)
        for stream in range(streams):
            mix = wide(mix_in[places, stream, :])
            q_all[stream, places, :head] = q_in[places, stream, :]
            q_all[stream, places, head:] = jnp.where(kept, mix, 0.0).astype(jnp.bfloat16)
            key_all[stream, places, :head] = nope_in[places, stream, :]
            key_all[stream, places, head:] = jnp.where(kept, turn(mix), 0.0).astype(
                jnp.bfloat16
            )
            value_all[stream, places, :] = value_in[places, stream, :]

    for copy in own:
        copy.wait()
    unpack(me)
    proj_serve(2)
    proj_serve(3)
    served = 4
    for offset in order:
        source = (me + peers - offset) % peers
        for which in range(4):
            src, dst = block_copies(source, own_places(source))[which]
            remote(
                src, dst, a_send.at[offset, which], a_recv.at[offset, which], plane, source
            ).wait_recv()
        unpack(source)
        if served < 8:
            proj_serve(served)
            served += 1
    while served < 12:
        proj_serve(served)
        served += 1

    scale = (NOPE + ROPE) ** (-0.5) * 1.4426950408889634
    query_rows = length // 4
    group = query_rows // block
    begins = [
        jnp.sum(1 - segments_ref[stream : stream + 1, :], axis=1, keepdims=True)
        for stream in range(streams)
    ]
    spot_row = lax.broadcasted_iota(jnp.int32, (block * streams, block * streams), 0)
    spot_column = lax.broadcasted_iota(jnp.int32, (block * streams, block * streams), 1)
    weave = jnp.where(
        spot_column == (spot_row % streams) * block + spot_row // streams, 1.0, 0.0
    ).astype(jnp.bfloat16)

    def b_copy(target):
        return remote(
            out_stage.at[target],
            attn.at[:, own_columns(me * head)],
            b_send.at[target],
            b_recv.at[me],
            plane,
            target,
        )

    for part in range(3, -1, -1):
        rows = pl.ds(part * query_rows, query_rows)
        seen = (part + 1) * query_rows
        outs = []
        for stream in range(streams):
            scores = lax.dot_general(
                q_all[stream, rows, :],
                key_all[stream, :seen, :],
                (((1,), (1,)), ((), ())),
                preferred_element_type=jnp.float32,
            )
            row_at = part * query_rows + lax.broadcasted_iota(jnp.int32, (query_rows, 1), 0)
            column_at = lax.broadcasted_iota(jnp.int32, (query_rows, seen), 1)
            first_key = jnp.where(row_at >= begins[stream], begins[stream], 0)
            allowed = (column_at <= row_at) & (column_at >= first_key)
            scores = jnp.where(allowed, scores, -jnp.inf)
            peak = jnp.max(scores, axis=1, keepdims=True)
            raised = jnp.exp2((scores - peak) * scale)
            total = jnp.sum(raised, axis=1, keepdims=True)
            mixed = jnp.dot(
                raised.astype(jnp.bfloat16),
                value_all[stream, :seen, :],
                preferred_element_type=jnp.float32,
            )
            outs.append((mixed / total).astype(jnp.bfloat16))
        for at in range(group):
            target = part * group + at
            both = jnp.concatenate(
                [out[at * block : (at + 1) * block, :] for out in outs], axis=0
            )
            out_stage[target] = jnp.dot(
                weave, both, preferred_element_type=jnp.float32
            ).astype(jnp.bfloat16)

            @pl.when(me != target)
            def _():
                b_copy(target).start()

            @pl.when(me == target)
            def _():
                pltpu.make_async_copy(
                    out_stage.at[target], attn.at[:, own_columns(me * head)], load_sem.at[7]
                ).start()

    while served < 16:
        proj_wait(served)
        start(
            proj_copy(4, served, *proj_source(served, me, plane))
        )
        served += 1
    load_proj.wait()
    for index in range(16):
        part, device = proj_source(index, mate, plane)
        proj_copy(4, index, part, device).wait_recv()

    for offset in order:
        source = (me + peers - offset) % peers
        remote(
            out_stage.at[source],
            attn.at[:, own_columns(source * head)],
            b_send.at[source],
            b_recv.at[source],
            plane,
            source,
        ).wait_recv()
    pltpu.make_async_copy(
        out_stage.at[me], attn.at[:, own_columns(me * head)], load_sem.at[7]
    ).wait()

    squares = jnp.zeros((block * streams, 1), jnp.float32)
    step = 4 * head
    for first in range(0, width, step):
        projected = jnp.dot(
            attn[...], proj[:, first : first + step], preferred_element_type=jnp.float32
        )
        before = jnp.concatenate(
            [
                residual_ref[:, :, at : at + head].reshape(block * streams, head)
                for at in range(first, first + step, head)
            ],
            axis=1,
        )
        hidden = before.astype(jnp.float32) + projected
        hidden_ref[:, first : first + step] = hidden
        squares = squares + jnp.sum(hidden * hidden, axis=1, keepdims=True)
    factor = lax.rsqrt(squares * (1.0 / width) + EPSILON)
    for first in range(0, width, step):
        gain = gain_ref[:, first : first + step].astype(jnp.float32)
        normed_ref[:, first : first + step] = (
            hidden_ref[:, first : first + step] * factor * gain
        ).astype(jnp.bfloat16)

    for copy in sent:
        copy.wait_send()
    for target in range(peers):

        @pl.when(me != target)
        def _():
            b_copy(target).wait_send()


def attend_and_project(
    queries, key_nope, key_rope, values, residual, segments, out_proj, norm_gain, peers
):
    block, streams, q_width = queries.shape
    width = residual.shape[2]
    tokens = block * streams
    length = block * peers
    vmem = pl.BlockSpec(memory_space=pltpu.VMEM)
    anywhere = pl.BlockSpec(memory_space=pl.ANY)
    dma = pltpu.SemaphoreType.DMA
    arrived = pltpu.VMEM((length, streams, NOPE), jnp.bfloat16)
    rope = jnp.pad(key_rope, ((0, 0), (0, 0), (0, NOPE - ROPE)))
    return pl.pallas_call(
        functools.partial(attention_kernel, peers),
        out_shape=(
            jax.ShapeDtypeStruct((tokens, width), jnp.float32),
            jax.ShapeDtypeStruct((tokens, width), jnp.bfloat16),
        ),
        in_specs=[anywhere, anywhere, anywhere, anywhere, vmem, vmem, anywhere, vmem],
        out_specs=(vmem, vmem),
        scratch_shapes=[
            pltpu.VMEM((block, streams, q_width), jnp.bfloat16),
            pltpu.VMEM((peers, block, streams, NOPE), jnp.bfloat16),
            pltpu.VMEM((peers + 1, block, streams, NOPE), jnp.bfloat16),
            arrived,
            arrived,
            arrived,
            arrived,
            pltpu.VMEM((streams, length, 2 * NOPE), jnp.bfloat16),
            pltpu.VMEM((streams, length, 2 * NOPE), jnp.bfloat16),
            pltpu.VMEM((streams, length, V_DIM), jnp.bfloat16),
            pltpu.VMEM((peers, tokens, V_DIM), jnp.bfloat16),
            pltpu.VMEM((tokens, HEADS * V_DIM), jnp.bfloat16),
            pltpu.VMEM((HEADS * V_DIM, width), jnp.bfloat16),
            dma((8,)),
            dma((peers, 4)),
            dma((peers, 4)),
            dma((peers,)),
            dma((peers,)),
            dma((5, 16)),
            dma((5, 16)),
        ],
        compiler_params=pltpu.CompilerParams(
            collective_id=0, has_side_effects=True, vmem_limit_bytes=64000000
        ),
    )(
        queries,
        key_nope,
        rope,
        values,
        residual,
        segments,
        out_proj,
        norm_gain.reshape(1, width),
    )


def attend_items(query_items, key_items, value_items, segment_items):
    length, count_items, qk_width = query_items.shape
    block_rows = QUERY_BLOCK
    score_scale = qk_width ** (-0.5)
    key_positions = jnp.arange(length, dtype=jnp.int32)

    def one_block(block_index):
        first_row = block_index * block_rows
        query_block = lax.dynamic_slice_in_dim(query_items, first_row, block_rows, 0)
        scores = (
            jnp.einsum("qid,kid->iqk", query_block, key_items, preferred_element_type=jnp.float32)
            * score_scale
        )
        row_positions = first_row + jnp.arange(block_rows, dtype=jnp.int32)
        row_segments = lax.dynamic_slice_in_dim(segment_items, first_row, block_rows, 1)
        allowed = (row_positions[None, :, None] >= key_positions[None, None, :]) & (
            row_segments[:, :, None] == segment_items[:, None, :]
        )
        scores = jnp.where(allowed, scores, -jnp.inf)
        row_peak = jnp.max(scores, axis=2, keepdims=True)
        raised = jnp.exp(scores - row_peak)
        weights = (raised / jnp.sum(raised, axis=2, keepdims=True)).astype(jnp.bfloat16)
        return jnp.einsum(
            "iqk,kid->qid", weights, value_items, preferred_element_type=jnp.float32
        ).astype(jnp.bfloat16)

    blocks = lax.map(one_block, jnp.arange(length // block_rows, dtype=jnp.int32))
    return blocks.reshape(length, count_items, value_items.shape[2])


def attend_by_heads(
    queries, key_nope, key_rope, values, residual, segments, out_proj, norm_gain, expert_count
):
    half_rows, stream_count, query_width = queries.shape
    model_width = residual.shape[2]
    token_rows = half_rows * stream_count
    item_count = stream_count * HEADS // expert_count
    key_heads = jnp.concatenate(
        [
            key_nope.reshape(half_rows, stream_count, HEADS, NOPE),
            jnp.broadcast_to(key_rope[:, :, None, :], (half_rows, stream_count, HEADS, ROPE)),
        ],
        axis=3,
    )
    query_items = queries.reshape(half_rows, stream_count * HEADS, NOPE + ROPE)
    key_items = key_heads.reshape(half_rows, stream_count * HEADS, NOPE + ROPE)
    value_items = values.reshape(half_rows, stream_count * HEADS, V_DIM)
    packed = jnp.concatenate([query_items, key_items, value_items], axis=2)
    packed_all = lax.all_to_all(packed, "expert", split_axis=1, concat_axis=0, tiled=True)
    qk_width = NOPE + ROPE
    query_all = packed_all[:, :, :qk_width]
    key_all = packed_all[:, :, qk_width : 2 * qk_width]
    value_all = packed_all[:, :, 2 * qk_width :]
    item_ids = lax.axis_index("expert") * item_count + jnp.arange(item_count, dtype=jnp.int32)
    stream_ids = item_ids // HEADS
    selector = (stream_ids[:, None] == jnp.arange(stream_count, dtype=jnp.int32)[None, :]).astype(
        jnp.int32
    )
    segment_items = jnp.sum(selector[:, :, None] * segments[None, :, :], axis=1)
    attended_items = attend_items(query_all, key_all, value_all, segment_items)
    attended_back = lax.all_to_all(
        attended_items, "expert", split_axis=0, concat_axis=1, tiled=True
    )
    attn_rows = attended_back.reshape(token_rows, HEADS * V_DIM)
    projected = jnp.dot(
        attn_rows,
        lax.all_gather(out_proj, ("dp", "expert"), axis=0, tiled=True),
        preferred_element_type=jnp.float32,
    )
    hidden = residual.reshape(token_rows, model_width).astype(jnp.float32) + projected
    mean_square = jnp.mean(hidden * hidden, axis=1, keepdims=True)
    normed = (hidden * lax.rsqrt(mean_square + EPSILON) * norm_gain.astype(jnp.float32)).astype(
        jnp.bfloat16
    )
    return hidden, normed


def body(
    queries,
    key_nope,
    key_rope,
    values,
    residual,
    segments,
    out_proj,
    norm_gain,
    expert_gate,
    expert_up,
    expert_down,
    routes,
    route_weights,
):
    half_rows, stream_count, query_width = queries.shape
    model_width = residual.shape[2]
    token_rows = half_rows * stream_count
    expert_count = lax.axis_size("expert")
    attend = attend_by_heads
    if expert_count == HEADS and lax.axis_size("dp") == 2 and stream_count == 2:
        attend = attend_and_project
    hidden, normed = attend(
        queries, key_nope, key_rope, values, residual, segments, out_proj, norm_gain, expert_count
    )
    token_routes = routes.reshape(token_rows, TOP)
    token_weights = route_weights.reshape(token_rows, TOP)
    expert_ids = jnp.arange(expert_count, dtype=jnp.int32)
    weight_table = jnp.sum(
        jnp.where(
            token_routes[:, :, None] == expert_ids[None, None, :], token_weights[:, :, None], 0.0
        ),
        axis=1,
    )
    layer_out = routed_experts(
        normed,
        weight_table.T,
        hidden,
        jnp.swapaxes(expert_gate[0], 0, 1),
        jnp.swapaxes(expert_up[0], 0, 1),
        expert_down[0],
    )
    return layer_out.reshape(half_rows, stream_count, model_width)


def solution(mesh):
    return jax.shard_map(
        body,
        mesh=mesh,
        in_specs=(
            P("expert", "dp", None),
            P("expert", "dp", None),
            P("expert", "dp", None),
            P("expert", "dp", None),
            P("expert", "dp", None),
            P("dp", None),
            P(("dp", "expert"), None),
            P(),
            P("expert", None, None),
            P("expert", None, None),
            P("expert", None, None),
            P("dp", "expert", None, None),
            P("dp", "expert", None, None),
        ),
        out_specs=P("expert", "dp", None),
        check_vma=False,
    )
```

```python
import functools

import jax
import jax.numpy as jnp
from jax import lax
from jax.experimental import pallas as pl
from jax.experimental.pallas import tpu as pltpu
from jax.sharding import PartitionSpec as P

HEADS = 16
NOPE = 128
ROPE = 64
V_DIM = 128
TOP = 6


EPSILON = 1e-06
QUERY_BLOCK = 512


MESH = pl.DeviceIdType.MESH


def ring_position(chip, chips):
    odd = chip % 2
    return (1 - odd) * (chip // 2) + odd * (chips - 1 - chip // 2)


def ring_chip(position, chips):
    back = position // (chips // 2)
    return (1 - back) * (2 * position) + back * (2 * (chips - 1 - position) + 1)


def expert_part(
    chips,
    alone,
    store,
    x_ref,
    table_ref,
    hidden_ref,
    gate_ref,
    up_ref,
    down_ref,
    rows_all,
    table_all,
    own_part,
    mate_part,
    ring_in,
    act,
    gate_vmem,
    up_vmem,
    down_vmem,
    weight_sem,
    x_send,
    x_recv,
    t_send,
    t_recv,
    m_send,
    m_recv,
    r_send,
    r_recv,
):
    tokens, width = x_ref.shape
    half = tokens // 2
    far = chips // 2
    me = lax.axis_index("expert")
    core = me % 2
    position = ring_position(me // 2, chips)
    after = 2 * ring_chip((position + 1) % chips, chips) + core
    before = 2 * ring_chip((position + chips - 1) % chips, chips) + core
    mate = me + 1 - 2 * core
    def slot_of(way, distance):
        if distance == 0:
            return 0
        if distance == far:
            return chips - 1
        return 2 * distance - 1 + way

    def reach(way, part):
        return far if part == way else far - 1

    targets = (after, before)

    if alone:
        barrier = pltpu.get_barrier_semaphore()
        for other in (after, before, mate):
            pl.semaphore_signal(barrier, inc=1, device_id={"expert": other}, device_id_type=MESH)

    loads = [
        pltpu.make_async_copy(src, dst, weight_sem.at[i])
        for i, (src, dst) in enumerate(
            ((gate_ref, gate_vmem), (up_ref, up_vmem), (down_ref, down_vmem))
        )
    ]
    for load in loads:
        load.start()
    if alone:
        pl.semaphore_wait(barrier, 3)
    yield

    def remote(src, dst, send, recv, other):
        return pltpu.make_async_remote_copy(
            src_ref=src,
            dst_ref=dst,
            send_sem=send,
            recv_sem=recv,
            device_id={"expert": other},
            device_id_type=MESH,
        )

    def rows_of(part):
        return pl.ds(part * half, half)

    def row_copy(way, distance, part):
        if way == 2:
            slot = distance
            src = x_ref.at[rows_of(part)] if slot == 0 else rows_all.at[slot, 0, rows_of(part)]
            dst = rows_all.at[slot, 1, rows_of(part)]
            other = mate
        else:
            slot = slot_of(way, distance)
            src = (
                x_ref.at[rows_of(part)]
                if distance == 1
                else rows_all.at[slot_of(way, distance - 1), 0, rows_of(part)]
            )
            dst = rows_all.at[slot, 0, rows_of(part)]
            other = targets[way]
        return remote(
            src, dst, x_send.at[way, distance, part], x_recv.at[way, distance, part], other
        )

    def table_copy(way, distance):
        if way == 2:
            slot = distance
            src = table_ref if slot == 0 else table_all.at[slot, 0]
            dst = table_all.at[slot, 1]
            other = mate
        else:
            slot = slot_of(way, distance)
            src = table_ref if distance == 1 else table_all.at[slot_of(way, distance - 1), 0]
            dst = table_all.at[slot, 0]
            other = targets[way]
        return remote(src, dst, t_send.at[way, distance], t_recv.at[way, distance], other)

    sent = []

    def start(copy):
        copy.start()
        sent.append(copy)

    def table_goes(way, distance):
        return distance < far or way == 0

    for part in range(2):
        for way in range(2):
            start(row_copy(way, 1, (part + way) % 2))
        start(row_copy(2, 0, part))
    for way in range(2):
        start(table_copy(way, 1))
    start(table_copy(2, 0))

    def serve(distance, turn):
        for way in range(2):
            part = (turn + way) % 2
            if distance > reach(way, part):
                continue
            row_copy(way, distance, part).wait_recv()
            if distance + 1 <= reach(way, part):
                start(row_copy(way, distance + 1, part))
            start(row_copy(2, slot_of(way, distance), part))
            if turn == 0 and table_goes(way, distance):
                table_copy(way, distance).wait_recv()
                if distance + 1 <= far and table_goes(way, distance + 1):
                    start(table_copy(way, distance + 1))
                start(table_copy(2, slot_of(way, distance)))

    def mate_copy(slot):
        return remote(
            rows_all.at[slot, 1], mate_part.at[slot], m_send.at[slot], m_recv.at[slot], mate
        )

    hidden_units = gate_vmem.shape[0]
    eye = lax.broadcasted_iota(jnp.int32, (tokens, tokens), 0) == lax.broadcasted_iota(
        jnp.int32, (tokens, tokens), 1
    )

    def column(row):
        return jnp.sum(jnp.where(eye, row, 0.0), axis=1, keepdims=True)

    def experts(slot):
        for part in range(2):
            row_copy(2, slot, part).wait_recv()
        table_copy(2, slot).wait_recv()
        mine = x_ref[...] if slot == 0 else rows_all[slot, 0]
        rows = jnp.concatenate([mine, rows_all[slot, 1]], axis=0)
        for first in range(0, hidden_units, 256):
            count = min(256, hidden_units - first)
            dims = (((1,), (1,)), ((), ()))
            gate_part = lax.dot_general(
                rows, gate_vmem[first : first + count, :], dims, preferred_element_type=jnp.float32
            )
            up_part = lax.dot_general(
                rows, up_vmem[first : first + count, :], dims, preferred_element_type=jnp.float32
            )
            silu = gate_part / (1.0 + jnp.exp(-gate_part))
            act[:, first : first + count] = (silu * up_part).astype(jnp.bfloat16)
        own_table = table_ref if slot == 0 else table_all.at[slot, 0]
        own_column = column(own_table[pl.ds(me, 1), :])
        mate_column = column(table_all[slot, 1, pl.ds(me, 1), :])
        for first in range(0, width, 512):
            y = jnp.dot(
                act[...], down_vmem[:, first : first + 512], preferred_element_type=jnp.float32
            )
            own_part[slot, :, first : first + 512] = (y[:tokens] * own_column).astype(jnp.bfloat16)
            rows_all[slot, 1, :, first : first + 512] = (y[tokens:] * mate_column).astype(
                jnp.bfloat16
            )
        start(mate_copy(slot))

    def sum_slot(way, distance):
        return slot_of(1 - way, distance)

    def sum_copy(way, distance, part):
        return remote(
            own_part.at[sum_slot(way, distance), rows_of(part)],
            ring_in.at[way, distance - 1, part],
            r_send.at[way, distance, part],
            r_recv.at[way, distance, part],
            targets[way],
        )

    mated = set()

    def mated_wait(slot):
        if slot not in mated:
            mated.add(slot)
            mate_copy(slot).wait_recv()

    def chip_sum(slot, part):
        mated_wait(slot)
        return own_part[slot, rows_of(part), :].astype(jnp.float32) + mate_part[
            slot, rows_of(part), :
        ].astype(jnp.float32)

    def send_sum(distance, late):
        for way in range(2):
            part = way if late else 1 - way
            if distance > reach(way, part):
                continue
            slot = sum_slot(way, distance)
            total = chip_sum(slot, part)
            if distance < reach(way, part):
                sum_copy(way, distance + 1, part).wait_recv()
                total = total + ring_in[way, distance, part].astype(jnp.float32)
            own_part[slot, rows_of(part), :] = total.astype(jnp.bfloat16)
            start(sum_copy(way, distance, part))

    for load in loads:
        load.wait()
    experts(0)
    serve(1, 0)
    serve(1, 1)
    for distance in range(1, far):
        experts(slot_of(0, distance))
        serve(distance + 1, 0)
        experts(slot_of(1, distance))
        if distance + 1 < far:
            serve(distance + 1, 1)
    send_sum(far - 1, False)
    experts(slot_of(0, far))
    send_sum(far, True)
    for distance in range(far - 2, 0, -1):
        send_sum(distance, False)
        send_sum(distance + 1, True)
    send_sum(1, True)
    for part in range(2):
        total = hidden_ref[rows_of(part), :] + chip_sum(0, part)
        for way in range(2):
            sum_copy(way, 1, part).wait_recv()
            total = total + ring_in[way, 0, part].astype(jnp.float32)
        store(part * half, total.astype(jnp.bfloat16))
    for copy in sent:
        copy.wait_send()
    yield


def expert_kernel(chips, x_ref, table_ref, hidden_ref, gate_ref, up_ref, down_ref, out_ref, *scratch):
    def store(first, rows):
        out_ref[pl.ds(first, rows.shape[0]), :] = rows

    part = expert_part(
        chips, True, store, x_ref, table_ref, hidden_ref, gate_ref, up_ref, down_ref, *scratch
    )
    next(part)
    next(part)


def expert_scratch(tokens, width, count, units):
    chips = count // 2
    half = tokens // 2
    far = chips // 2
    dma = pltpu.SemaphoreType.DMA
    return [
        pltpu.VMEM((chips, 2, tokens, width), jnp.bfloat16),
        pltpu.VMEM((chips, 2, count, tokens), jnp.float32),
        pltpu.VMEM((chips, tokens, width), jnp.bfloat16),
        pltpu.VMEM((chips, tokens, width), jnp.bfloat16),
        pltpu.VMEM((2, far, 2, half, width), jnp.bfloat16),
        pltpu.VMEM((2 * tokens, units), jnp.bfloat16),
        pltpu.VMEM((units, width), jnp.bfloat16),
        pltpu.VMEM((units, width), jnp.bfloat16),
        pltpu.VMEM((units, width), jnp.bfloat16),
        dma((3,)),
        dma((3, chips, 2)),
        dma((3, chips, 2)),
        dma((3, chips)),
        dma((3, chips)),
        dma((chips,)),
        dma((chips,)),
        dma((2, far + 1, 2)),
        dma((2, far + 1, 2)),
    ]

def routed_experts(normed, table, hidden, gate, up, down):
    tokens, width = normed.shape
    count = table.shape[0]
    chips = count // 2
    units = gate.shape[0]
    vmem = pl.BlockSpec(memory_space=pltpu.VMEM)
    anywhere = pl.BlockSpec(memory_space=pl.ANY)
    return pl.pallas_call(
        functools.partial(expert_kernel, chips),
        out_shape=jax.ShapeDtypeStruct((tokens, width), jnp.bfloat16),
        in_specs=[vmem, vmem, vmem, anywhere, anywhere, anywhere],
        out_specs=vmem,
        scratch_shapes=expert_scratch(tokens, width, count, units),
        compiler_params=pltpu.CompilerParams(
            collective_id=1, has_side_effects=True, vmem_limit_bytes=64000000
        ),
    )(normed, table, hidden, gate, up, down)


def flip(device, bit):
    return device + bit - 2 * bit * ((device // bit) % 2)


def attention_part(
    peers,
    q_ref,
    nope_ref,
    rope_ref,
    value_ref,
    residual_ref,
    segments_ref,
    proj_ref,
    gain_ref,
    hidden_ref,
    normed_ref,
    q_own,
    rope_own,
    stage,
    arrived,
    q_all,
    key_all,
    value_all,
    out_stage,
    attn,
    proj,
    load_sem,
    stage_sem,
    a_send,
    a_recv,
    b_send,
    b_recv,
    c_send,
    c_recv,
):
    block, streams, _ = q_ref.shape
    length = block * peers
    head = NOPE
    width = proj_ref.shape[1]
    proj_rows = proj_ref.shape[0]
    me = lax.axis_index("expert")
    plane = lax.axis_index("dp")
    mate, row_mate = flip(me, 1), flip(me, 2)
    near, far = flip(me, peers // 4), flip(me, peers // 2)

    barrier = pltpu.get_barrier_semaphore()
    for offset in range(1, peers):
        pl.semaphore_signal(
            barrier,
            inc=1,
            device_id={"dp": plane, "expert": (me + offset) % peers},
            device_id_type=MESH,
        )
    pl.semaphore_signal(
        barrier, inc=1, device_id={"dp": 1 - plane, "expert": me}, device_id_type=MESH
    )

    def own_places(device):
        return pl.ds(pl.multiple_of(device * block, block), block)

    def proj_place(part, device):
        return pl.ds(
            pl.multiple_of((part * peers + device) * proj_rows, proj_rows), proj_rows
        )

    load_q = pltpu.make_async_copy(q_ref, q_own, load_sem.at[0])
    load_rope = pltpu.make_async_copy(rope_ref, rope_own, load_sem.at[1])
    load_proj = pltpu.make_async_copy(
        proj_ref, proj.at[proj_place(plane, me)], load_sem.at[2]
    )
    staged = [
        pltpu.make_async_copy(
            src.at[:, :, target * head : (target + 1) * head],
            stage.at[target, 2 + i],
            stage_sem.at[target, i],
        )
        for target in range(peers)
        for i, src in enumerate((nope_ref, value_ref))
    ]
    for load in [load_q, load_rope, load_proj] + staged:
        load.start()
    pl.semaphore_wait(barrier, peers)

    def remote(src, dst, send, recv, part, other):
        return pltpu.make_async_remote_copy(
            src_ref=src,
            dst_ref=dst,
            send_sem=send,
            recv_sem=recv,
            device_id={"dp": part, "expert": other},
            device_id_type=MESH,
        )

    sent = []

    def start(copy):
        copy.start()
        sent.append(copy)

    partners = (
        (plane, far),
        (plane, near),
        (plane, row_mate),
        (1 - plane, me),
        (plane, mate),
    )

    def proj_copy(stage, index, src_part, src_device, from_input=False):
        place = proj.at[proj_place(src_part, src_device)]
        part, other = partners[stage]
        return remote(
            proj_ref if from_input else place,
            place,
            c_send.at[stage, index],
            c_recv.at[stage, index],
            part,
            other,
        )

    def proj_source(index, of_device, of_part):
        device = of_device
        if index & 1:
            device = flip(device, peers // 2)
        if index & 2:
            device = flip(device, peers // 4)
        if index & 4:
            device = flip(device, 2)
        return (1 - of_part if index & 8 else of_part), device

    def proj_forward(index):
        first = index.bit_length()
        part, device = proj_source(index, me, plane)
        for stage in range(first, 5):
            start(proj_copy(stage, index, part, device, from_input=index == 0))

    def proj_wait(index):
        stage = index.bit_length() - 1
        part, device = proj_source(index, me, plane)
        proj_copy(stage, index - (1 << stage), part, device).wait_recv()

    def proj_serve(index):
        proj_wait(index)
        proj_forward(index)

    proj_forward(0)

    def a_copy(offset, source, target):
        return remote(
            stage.at[target],
            arrived.at[source],
            a_send.at[offset],
            a_recv.at[offset],
            plane,
            target if source is me else source,
        )

    order = sorted(range(1, peers), key=lambda offset: (abs(offset - peers // 2), offset))

    load_q.wait()
    load_rope.wait()
    lane = lax.broadcasted_iota(jnp.int32, (block * streams, head), 1)
    low = lane < ROPE

    def wide(x):
        return x.astype(jnp.float32)

    def turn(x):
        return pltpu.roll(x, ROPE, 1)

    rope_once = wide(rope_own[...]).reshape(block * streams, ROPE)
    rope_twice = jnp.concatenate([rope_once, rope_once], axis=1)
    for pair in range(HEADS // 2):
        first = pair * 3 * head
        one, two, three = (
            q_own[:, :, first + i * head : first + (i + 1) * head].reshape(block * streams, head)
            for i in range(3)
        )
        two, three = wide(two), wide(three)
        shape = (block, streams, head)

        def narrow(x):
            return x.astype(jnp.bfloat16).reshape(shape)

        stage[2 * pair, 0] = one.reshape(shape)
        stage[2 * pair, 1] = narrow(jnp.where(low, two, rope_twice))
        stage[2 * pair + 1, 0] = narrow(turn(jnp.where(low, three, two)))
        stage[2 * pair + 1, 1] = narrow(jnp.where(low, rope_twice, three))
    for load in staged:
        load.wait()
    for offset in order[:4]:
        start(a_copy(offset, me, (me + offset) % peers))
    proj_serve(1)
    for offset in order[4:]:
        start(a_copy(offset, me, (me + offset) % peers))

    odd = jnp.full((block, head), me % 2, jnp.int32)
    here = lax.broadcasted_iota(jnp.int32, (block, head), 1) // ROPE
    kept = here == odd

    def unpack(blocks, device):
        places = own_places(device)
        for stream in range(streams):
            mix = wide(blocks[device, 1, :, stream, :])
            q_all[stream, places, :head] = blocks[device, 0, :, stream, :]
            q_all[stream, places, head:] = jnp.where(kept, mix, 0.0).astype(jnp.bfloat16)
            key_all[stream, places, :head] = blocks[device, 2, :, stream, :]
            key_all[stream, places, head:] = jnp.where(kept, turn(mix), 0.0).astype(jnp.bfloat16)
            value_all[stream, places, :] = blocks[device, 3, :, stream, :]

    unpack(stage, me)
    proj_serve(2)
    proj_serve(3)
    served = 4
    for offset in order:
        source = (me + peers - offset) % peers
        a_copy(offset, source, me).wait_recv()
        unpack(arrived, source)
        if served < 12:
            proj_serve(served)
            served += 1

    scale = (NOPE + ROPE) ** (-0.5) * 1.4426950408889634
    query_rows = length // 4
    group = query_rows // block
    begins = [
        jnp.sum(1 - segments_ref[stream : stream + 1, :], axis=1, keepdims=True)
        for stream in range(streams)
    ]
    spot_row = lax.broadcasted_iota(jnp.int32, (block * streams, block * streams), 0)
    spot_column = lax.broadcasted_iota(jnp.int32, (block * streams, block * streams), 1)
    weave = jnp.where(
        spot_column == (spot_row % streams) * block + spot_row // streams, 1.0, 0.0
    ).astype(jnp.bfloat16)

    def b_copy(target):
        return remote(
            out_stage.at[target],
            attn.at[me],
            b_send.at[target],
            b_recv.at[me],
            plane,
            target,
        )

    for part in range(3, -1, -1):
        rows = pl.ds(part * query_rows, query_rows)
        seen = (part + 1) * query_rows
        outs = []
        for stream in range(streams):
            scores = lax.dot_general(
                q_all[stream, rows, :],
                key_all[stream, :seen, :],
                (((1,), (1,)), ((), ())),
                preferred_element_type=jnp.float32,
            )
            row_at = part * query_rows + lax.broadcasted_iota(jnp.int32, (query_rows, 1), 0)
            column_at = lax.broadcasted_iota(jnp.int32, (query_rows, seen), 1)
            first_key = jnp.where(row_at >= begins[stream], begins[stream], 0)
            allowed = (column_at <= row_at) & (column_at >= first_key)
            scores = jnp.where(allowed, scores, -jnp.inf)
            peak = jnp.max(scores, axis=1, keepdims=True)
            raised = jnp.exp2((scores - peak) * scale)
            total = jnp.sum(raised, axis=1, keepdims=True)
            mixed = jnp.dot(
                raised.astype(jnp.bfloat16),
                value_all[stream, :seen, :],
                preferred_element_type=jnp.float32,
            )
            outs.append((mixed / total).astype(jnp.bfloat16))
        for at in range(group):
            target = part * group + at
            both = jnp.concatenate(
                [out[at * block : (at + 1) * block, :] for out in outs], axis=0
            )
            out_stage[target] = jnp.dot(
                weave, both, preferred_element_type=jnp.float32
            ).astype(jnp.bfloat16)

            @pl.when(me != target)
            def _():
                b_copy(target).start()

            @pl.when(me == target)
            def _():
                attn[target] = out_stage[target]

    while served < 16:
        proj_wait(served)
        start(
            proj_copy(4, served, *proj_source(served, me, plane))
        )
        served += 1
    load_proj.wait()
    for index in range(16):
        part, device = proj_source(index, mate, plane)
        proj_copy(4, index, part, device).wait_recv()

    for offset in order:
        source = (me + peers - offset) % peers
        remote(
            out_stage.at[source],
            attn.at[source],
            b_send.at[source],
            b_recv.at[source],
            plane,
            source,
        ).wait_recv()
    mixed_rows = jnp.concatenate([attn[at] for at in range(peers)], axis=1)
    squares = jnp.zeros((block * streams, 1), jnp.float32)
    step = 4 * head
    for first in range(0, width, step):
        projected = jnp.dot(
            mixed_rows, proj[:, first : first + step], preferred_element_type=jnp.float32
        )
        before = jnp.concatenate(
            [
                residual_ref[:, :, at : at + head].reshape(block * streams, head)
                for at in range(first, first + step, head)
            ],
            axis=1,
        )
        hidden = before.astype(jnp.float32) + projected
        hidden_ref[:, first : first + step] = hidden
        squares = squares + jnp.sum(hidden * hidden, axis=1, keepdims=True)
    factor = lax.rsqrt(squares * (1.0 / width) + EPSILON)
    for first in range(0, width, step):
        gain = gain_ref[:, first : first + step].astype(jnp.float32)
        normed_ref[:, first : first + step] = (
            hidden_ref[:, first : first + step] * factor * gain
        ).astype(jnp.bfloat16)

    yield
    for copy in sent:
        copy.wait_send()
    for target in range(peers):

        @pl.when(me != target)
        def _():
            b_copy(target).wait_send()
    yield


def layer_kernel(
    peers,
    q_ref,
    nope_ref,
    rope_ref,
    value_ref,
    residual_ref,
    segments_ref,
    proj_ref,
    gain_ref,
    routes_ref,
    weights_ref,
    gate_ref,
    up_ref,
    down_ref,
    out_ref,
    hidden,
    normed,
    table,
    *scratch,
):
    block, streams, width = out_ref.shape
    split = 18
    attention = attention_part(
        peers,
        q_ref,
        nope_ref,
        rope_ref,
        value_ref,
        residual_ref,
        segments_ref,
        proj_ref,
        gain_ref,
        hidden,
        normed,
        *scratch[:split],
    )

    def store(first, rows):
        count = rows.shape[0] // streams
        for at in range(0, width, NOPE):
            out_ref[pl.ds(first // streams, count), :, at : at + NOPE] = rows[
                :, at : at + NOPE
            ].reshape(count, streams, NOPE)

    experts = expert_part(
        peers // 2,
        False,
        store,
        normed,
        table,
        hidden,
        gate_ref,
        up_ref,
        down_ref,
        *scratch[split:],
    )
    choices, tokens = routes_ref.shape[0], routes_ref.shape[2]
    ids = lax.broadcasted_iota(jnp.int32, (peers, tokens), 0)
    sums = jnp.zeros((peers, tokens), jnp.float32)
    for at in range(choices):
        sums = sums + jnp.where(ids == routes_ref[at], weights_ref[at], 0.0)
    table[...] = sums
    next(experts)
    next(attention)
    next(experts)
    next(attention)


def whole_layer(
    queries,
    key_nope,
    key_rope,
    values,
    residual,
    segments,
    out_proj,
    norm_gain,
    routes,
    route_weights,
    gate,
    up,
    down,
    peers,
):
    block, streams, q_width = queries.shape
    width = residual.shape[2]
    tokens = block * streams
    length = block * peers
    vmem = pl.BlockSpec(memory_space=pltpu.VMEM)
    anywhere = pl.BlockSpec(memory_space=pl.ANY)
    dma = pltpu.SemaphoreType.DMA
    blocks = pltpu.VMEM((peers, 4, block, streams, NOPE), jnp.bfloat16)
    attention_scratch = [
        pltpu.VMEM((block, streams, q_width), jnp.bfloat16),
        pltpu.VMEM((block, streams, ROPE), jnp.bfloat16),
        blocks,
        blocks,
        pltpu.VMEM((streams, length, 2 * NOPE), jnp.bfloat16),
        pltpu.VMEM((streams, length, 2 * NOPE), jnp.bfloat16),
        pltpu.VMEM((streams, length, V_DIM), jnp.bfloat16),
        pltpu.VMEM((peers, tokens, V_DIM), jnp.bfloat16),
        pltpu.VMEM((peers, tokens, V_DIM), jnp.bfloat16),
        pltpu.VMEM((HEADS * V_DIM, width), jnp.bfloat16),
        dma((3,)),
        dma((peers, 2)),
        dma((peers,)),
        dma((peers,)),
        dma((peers,)),
        dma((peers,)),
        dma((5, 16)),
        dma((5, 16)),
    ]
    return pl.pallas_call(
        functools.partial(layer_kernel, peers),
        out_shape=jax.ShapeDtypeStruct((block, streams, width), jnp.bfloat16),
        in_specs=[anywhere] * 4 + [vmem, vmem, anywhere, vmem, vmem, vmem] + [anywhere] * 3,
        out_specs=vmem,
        scratch_shapes=[
            pltpu.VMEM((tokens, width), jnp.float32),
            pltpu.VMEM((tokens, width), jnp.bfloat16),
            pltpu.VMEM((peers, tokens), jnp.float32),
        ]
        + attention_scratch
        + expert_scratch(tokens, width, peers, gate.shape[0]),
        compiler_params=pltpu.CompilerParams(
            collective_id=0, has_side_effects=True, vmem_limit_bytes=64000000
        ),
    )(
        queries,
        key_nope,
        key_rope,
        values,
        residual,
        segments,
        out_proj,
        norm_gain.reshape(1, width),
        jnp.transpose(routes, (3, 0, 1, 2)).reshape(-1, 1, tokens),
        jnp.transpose(route_weights, (3, 0, 1, 2)).reshape(-1, 1, tokens),
        gate,
        up,
        down,
    )


def attend_items(query_items, key_items, value_items, segment_items):
    length, count_items, qk_width = query_items.shape
    block_rows = QUERY_BLOCK
    score_scale = qk_width ** (-0.5)
    key_positions = jnp.arange(length, dtype=jnp.int32)

    def one_block(block_index):
        first_row = block_index * block_rows
        query_block = lax.dynamic_slice_in_dim(query_items, first_row, block_rows, 0)
        scores = (
            jnp.einsum("qid,kid->iqk", query_block, key_items, preferred_element_type=jnp.float32)
            * score_scale
        )
        row_positions = first_row + jnp.arange(block_rows, dtype=jnp.int32)
        row_segments = lax.dynamic_slice_in_dim(segment_items, first_row, block_rows, 1)
        allowed = (row_positions[None, :, None] >= key_positions[None, None, :]) & (
            row_segments[:, :, None] == segment_items[:, None, :]
        )
        scores = jnp.where(allowed, scores, -jnp.inf)
        row_peak = jnp.max(scores, axis=2, keepdims=True)
        raised = jnp.exp(scores - row_peak)
        weights = (raised / jnp.sum(raised, axis=2, keepdims=True)).astype(jnp.bfloat16)
        return jnp.einsum(
            "iqk,kid->qid", weights, value_items, preferred_element_type=jnp.float32
        ).astype(jnp.bfloat16)

    blocks = lax.map(one_block, jnp.arange(length // block_rows, dtype=jnp.int32))
    return blocks.reshape(length, count_items, value_items.shape[2])


def attend_by_heads(
    queries, key_nope, key_rope, values, residual, segments, out_proj, norm_gain, expert_count
):
    half_rows, stream_count, query_width = queries.shape
    model_width = residual.shape[2]
    token_rows = half_rows * stream_count
    item_count = stream_count * HEADS // expert_count
    key_heads = jnp.concatenate(
        [
            key_nope.reshape(half_rows, stream_count, HEADS, NOPE),
            jnp.broadcast_to(key_rope[:, :, None, :], (half_rows, stream_count, HEADS, ROPE)),
        ],
        axis=3,
    )
    query_items = queries.reshape(half_rows, stream_count * HEADS, NOPE + ROPE)
    key_items = key_heads.reshape(half_rows, stream_count * HEADS, NOPE + ROPE)
    value_items = values.reshape(half_rows, stream_count * HEADS, V_DIM)
    packed = jnp.concatenate([query_items, key_items, value_items], axis=2)
    packed_all = lax.all_to_all(packed, "expert", split_axis=1, concat_axis=0, tiled=True)
    qk_width = NOPE + ROPE
    query_all = packed_all[:, :, :qk_width]
    key_all = packed_all[:, :, qk_width : 2 * qk_width]
    value_all = packed_all[:, :, 2 * qk_width :]
    item_ids = lax.axis_index("expert") * item_count + jnp.arange(item_count, dtype=jnp.int32)
    stream_ids = item_ids // HEADS
    selector = (stream_ids[:, None] == jnp.arange(stream_count, dtype=jnp.int32)[None, :]).astype(
        jnp.int32
    )
    segment_items = jnp.sum(selector[:, :, None] * segments[None, :, :], axis=1)
    attended_items = attend_items(query_all, key_all, value_all, segment_items)
    attended_back = lax.all_to_all(
        attended_items, "expert", split_axis=0, concat_axis=1, tiled=True
    )
    attn_rows = attended_back.reshape(token_rows, HEADS * V_DIM)
    projected = jnp.dot(
        attn_rows,
        lax.all_gather(out_proj, ("dp", "expert"), axis=0, tiled=True),
        preferred_element_type=jnp.float32,
    )
    hidden = residual.reshape(token_rows, model_width).astype(jnp.float32) + projected
    mean_square = jnp.mean(hidden * hidden, axis=1, keepdims=True)
    normed = (hidden * lax.rsqrt(mean_square + EPSILON) * norm_gain.astype(jnp.float32)).astype(
        jnp.bfloat16
    )
    return hidden, normed


def body(
    queries,
    key_nope,
    key_rope,
    values,
    residual,
    segments,
    out_proj,
    norm_gain,
    expert_gate,
    expert_up,
    expert_down,
    routes,
    route_weights,
):
    half_rows, stream_count, query_width = queries.shape
    model_width = residual.shape[2]
    token_rows = half_rows * stream_count
    expert_count = lax.axis_size("expert")
    gate = jnp.swapaxes(expert_gate[0], 0, 1)
    up = jnp.swapaxes(expert_up[0], 0, 1)
    attention_inputs = (
        queries,
        key_nope,
        key_rope,
        values,
        residual,
        segments,
        out_proj,
        norm_gain,
    )
    if expert_count == HEADS and lax.axis_size("dp") == 2 and stream_count == 2:
        return whole_layer(
            *attention_inputs, routes, route_weights, gate, up, expert_down[0], expert_count
        )
    hidden, normed = attend_by_heads(*attention_inputs, expert_count)
    token_routes = routes.reshape(token_rows, TOP)
    token_weights = route_weights.reshape(token_rows, TOP)
    expert_ids = jnp.arange(expert_count, dtype=jnp.int32)
    weight_table = jnp.sum(
        jnp.where(
            token_routes[:, :, None] == expert_ids[None, None, :], token_weights[:, :, None], 0.0
        ),
        axis=1,
    )
    layer_out = routed_experts(
        normed, weight_table.T, hidden, gate, up, expert_down[0]
    )
    return layer_out.reshape(half_rows, stream_count, model_width)


def solution(mesh):
    return jax.shard_map(
        body,
        mesh=mesh,
        in_specs=(
            P("expert", "dp", None),
            P("expert", "dp", None),
            P("expert", "dp", None),
            P("expert", "dp", None),
            P("expert", "dp", None),
            P("dp", None),
            P(("dp", "expert"), None),
            P(),
            P("expert", None, None),
            P("expert", None, None),
            P("expert", None, None),
            P("dp", "expert", None, None),
            P("dp", "expert", None, None),
        ),
        out_specs=P("expert", "dp", None),
        check_vma=False,
    )
```

```python
import functools

import jax
import jax.numpy as jnp
from jax import lax
from jax.experimental import pallas as pl
from jax.experimental.pallas import tpu as pltpu
from jax.sharding import PartitionSpec as P

HEADS = 16
NOPE = 128
ROPE = 64
V_DIM = 128
TOP = 6


EPSILON = 1e-06
FAR_BELOW = -1048576.0
QUERY_BLOCK = 512


MESH = pl.DeviceIdType.MESH


def ring_position(chip, chips):
    odd = chip % 2
    return (1 - odd) * (chip // 2) + odd * (chips - 1 - chip // 2)


def ring_chip(position, chips):
    back = position // (chips // 2)
    return (1 - back) * (2 * position) + back * (2 * (chips - 1 - position) + 1)


def expert_part(
    chips,
    alone,
    store,
    x_ref,
    table_ref,
    hidden_ref,
    gate_ref,
    up_ref,
    down_ref,
    rows_all,
    table_all,
    own_part,
    mate_part,
    ring_in,
    act,
    gate_vmem,
    up_vmem,
    down_vmem,
    weight_sem,
    x_send,
    x_recv,
    t_send,
    t_recv,
    m_send,
    m_recv,
    r_send,
    r_recv,
):
    tokens, width = x_ref.shape
    half = tokens // 2
    far = chips // 2
    me = lax.axis_index("expert")
    core = me % 2
    position = ring_position(me // 2, chips)
    after = 2 * ring_chip((position + 1) % chips, chips) + core
    before = 2 * ring_chip((position + chips - 1) % chips, chips) + core
    mate = me + 1 - 2 * core
    def slot_of(way, distance):
        if distance == 0:
            return 0
        if distance == far:
            return chips - 1
        return 2 * distance - 1 + way

    def reach(way, part):
        return far if part == way else far - 1

    targets = (after, before)

    if alone:
        barrier = pltpu.get_barrier_semaphore()
        for other in (after, before, mate):
            pl.semaphore_signal(barrier, inc=1, device_id={"expert": other}, device_id_type=MESH)

    loads = [
        pltpu.make_async_copy(src, dst, weight_sem.at[i])
        for i, (src, dst) in enumerate(
            ((gate_ref, gate_vmem), (up_ref, up_vmem), (down_ref, down_vmem))
        )
    ]
    for load in loads:
        load.start()
    if alone:
        pl.semaphore_wait(barrier, 3)
    yield

    def remote(src, dst, send, recv, other):
        return pltpu.make_async_remote_copy(
            src_ref=src,
            dst_ref=dst,
            send_sem=send,
            recv_sem=recv,
            device_id={"expert": other},
            device_id_type=MESH,
        )

    def rows_of(part):
        return pl.ds(part * half, half)

    def row_copy(way, distance, part):
        if way == 2:
            slot = distance
            src = x_ref.at[rows_of(part)] if slot == 0 else rows_all.at[slot, 0, rows_of(part)]
            dst = rows_all.at[slot, 1, rows_of(part)]
            other = mate
        else:
            slot = slot_of(way, distance)
            src = (
                x_ref.at[rows_of(part)]
                if distance == 1
                else rows_all.at[slot_of(way, distance - 1), 0, rows_of(part)]
            )
            dst = rows_all.at[slot, 0, rows_of(part)]
            other = targets[way]
        return remote(
            src, dst, x_send.at[way, distance, part], x_recv.at[way, distance, part], other
        )

    def table_copy(way, distance):
        if way == 2:
            slot = distance
            src = table_ref if slot == 0 else table_all.at[slot, 0]
            dst = table_all.at[slot, 1]
            other = mate
        else:
            slot = slot_of(way, distance)
            src = table_ref if distance == 1 else table_all.at[slot_of(way, distance - 1), 0]
            dst = table_all.at[slot, 0]
            other = targets[way]
        return remote(src, dst, t_send.at[way, distance], t_recv.at[way, distance], other)

    sent = []

    def start(copy):
        copy.start()
        sent.append(copy)

    def table_goes(way, distance):
        return distance < far or way == 0

    for part in range(2):
        for way in range(2):
            start(row_copy(way, 1, (part + way) % 2))
        start(row_copy(2, 0, part))
    for way in range(2):
        start(table_copy(way, 1))
    start(table_copy(2, 0))

    def serve(distance, turn):
        for way in range(2):
            part = (turn + way) % 2
            if distance > reach(way, part):
                continue
            row_copy(way, distance, part).wait_recv()
            if distance + 1 <= reach(way, part):
                start(row_copy(way, distance + 1, part))
            start(row_copy(2, slot_of(way, distance), part))
            if turn == 0 and table_goes(way, distance):
                table_copy(way, distance).wait_recv()
                if distance + 1 <= far and table_goes(way, distance + 1):
                    start(table_copy(way, distance + 1))
                start(table_copy(2, slot_of(way, distance)))

    def mate_copy(slot, part):
        return remote(
            rows_all.at[slot, 1, rows_of(part)],
            mate_part.at[slot, rows_of(part)],
            m_send.at[slot, part],
            m_recv.at[slot, part],
            mate,
        )

    hidden_units = gate_vmem.shape[0]
    eye = lax.broadcasted_iota(jnp.int32, (tokens, tokens), 0) == lax.broadcasted_iota(
        jnp.int32, (tokens, tokens), 1
    )

    def column(row):
        return jnp.sum(jnp.where(eye, row, 0.0), axis=1, keepdims=True)

    tabled = {}

    def columns_of(slot):
        if slot not in tabled:
            table_copy(2, slot).wait_recv()
            own_table = table_ref if slot == 0 else table_all.at[slot, 0]
            tabled[slot] = (
                column(own_table[pl.ds(me, 1), :]),
                column(table_all[slot, 1, pl.ds(me, 1), :]),
            )
        return tabled[slot]

    def experts(pieces):
        rows = []
        for slot, part in pieces:
            row_copy(2, slot, part).wait_recv()
            rows.append(x_ref[rows_of(part), :] if slot == 0 else rows_all[slot, 0, rows_of(part), :])
            rows.append(rows_all[slot, 1, rows_of(part), :])
        rows = jnp.concatenate(rows, axis=0)
        for first in range(0, hidden_units, 256):
            count = min(256, hidden_units - first)
            dims = (((1,), (1,)), ((), ()))
            gate_part = lax.dot_general(
                rows, gate_vmem[first : first + count, :], dims, preferred_element_type=jnp.float32
            )
            up_part = lax.dot_general(
                rows, up_vmem[first : first + count, :], dims, preferred_element_type=jnp.float32
            )
            silu = gate_part / (1.0 + jnp.exp(-gate_part))
            act[:, first : first + count] = (silu * up_part).astype(jnp.bfloat16)
        scales = [
            scale[part * half : (part + 1) * half]
            for slot, part in pieces
            for scale in columns_of(slot)
        ]
        for first in range(0, width, 512):
            columns = slice(first, first + 512)
            y = jnp.dot(act[...], down_vmem[:, columns], preferred_element_type=jnp.float32)
            for at, (slot, part) in enumerate(pieces):
                for side, place in enumerate((own_part.at[slot], rows_all.at[slot, 1])):
                    piece = 2 * at + side
                    place[rows_of(part), columns] = (
                        y[piece * half : (piece + 1) * half] * scales[piece]
                    ).astype(jnp.bfloat16)
        for slot, part in pieces:
            start(mate_copy(slot, part))

    def sum_slot(way, distance):
        return slot_of(1 - way, distance)

    def sum_copy(way, distance, part):
        return remote(
            own_part.at[sum_slot(way, distance), rows_of(part)],
            ring_in.at[way, distance - 1, part],
            r_send.at[way, distance, part],
            r_recv.at[way, distance, part],
            targets[way],
        )

    def chip_sum(slot, part):
        mate_copy(slot, part).wait_recv()
        return own_part[slot, rows_of(part), :].astype(jnp.float32) + mate_part[
            slot, rows_of(part), :
        ].astype(jnp.float32)

    def send_sum(distance, late):
        for way in range(2):
            part = way if late else 1 - way
            if distance > reach(way, part):
                continue
            slot = sum_slot(way, distance)
            total = chip_sum(slot, part)
            if distance < reach(way, part):
                sum_copy(way, distance + 1, part).wait_recv()
                total = total + ring_in[way, distance, part].astype(jnp.float32)
            own_part[slot, rows_of(part), :] = total.astype(jnp.bfloat16)
            start(sum_copy(way, distance, part))

    for load in loads:
        load.wait()
    experts(((0, 0), (0, 1)))
    for distance in range(1, far):
        for turn in range(2):
            serve(distance, turn)
            experts(((slot_of(0, distance), turn), (slot_of(1, distance), 1 - turn)))
            if distance == far - 1 and turn == 0:
                send_sum(distance, False)
    serve(far, 0)
    experts(((slot_of(0, far), 0), (slot_of(0, far), 1)))
    send_sum(far, True)
    for distance in range(far - 2, 0, -1):
        send_sum(distance, False)
        send_sum(distance + 1, True)
    send_sum(1, True)
    for part in range(2):
        total = hidden_ref[rows_of(part), :] + chip_sum(0, part)
        for way in range(2):
            sum_copy(way, 1, part).wait_recv()
            total = total + ring_in[way, 0, part].astype(jnp.float32)
        store(part * half, total.astype(jnp.bfloat16))
    for copy in sent:
        copy.wait_send()
    yield


def expert_kernel(chips, x_ref, table_ref, hidden_ref, gate_ref, up_ref, down_ref, out_ref, *scratch):
    def store(first, rows):
        out_ref[pl.ds(first, rows.shape[0]), :] = rows

    part = expert_part(
        chips, True, store, x_ref, table_ref, hidden_ref, gate_ref, up_ref, down_ref, *scratch
    )
    next(part)
    next(part)


def expert_scratch(tokens, width, count, units):
    chips = count // 2
    half = tokens // 2
    far = chips // 2
    dma = pltpu.SemaphoreType.DMA
    return [
        pltpu.VMEM((chips, 2, tokens, width), jnp.bfloat16),
        pltpu.VMEM((chips, 2, count, tokens), jnp.float32),
        pltpu.VMEM((chips, tokens, width), jnp.bfloat16),
        pltpu.VMEM((chips, tokens, width), jnp.bfloat16),
        pltpu.VMEM((2, far, 2, half, width), jnp.bfloat16),
        pltpu.VMEM((2 * tokens, units), jnp.bfloat16),
        pltpu.VMEM((units, width), jnp.bfloat16),
        pltpu.VMEM((units, width), jnp.bfloat16),
        pltpu.VMEM((units, width), jnp.bfloat16),
        dma((3,)),
        dma((3, chips, 2)),
        dma((3, chips, 2)),
        dma((3, chips)),
        dma((3, chips)),
        dma((chips, 2)),
        dma((chips, 2)),
        dma((2, far + 1, 2)),
        dma((2, far + 1, 2)),
    ]

def routed_experts(normed, table, hidden, gate, up, down):
    tokens, width = normed.shape
    count = table.shape[0]
    chips = count // 2
    units = gate.shape[0]
    vmem = pl.BlockSpec(memory_space=pltpu.VMEM)
    anywhere = pl.BlockSpec(memory_space=pl.ANY)
    return pl.pallas_call(
        functools.partial(expert_kernel, chips),
        out_shape=jax.ShapeDtypeStruct((tokens, width), jnp.bfloat16),
        in_specs=[vmem, vmem, vmem, anywhere, anywhere, anywhere],
        out_specs=vmem,
        scratch_shapes=expert_scratch(tokens, width, count, units),
        compiler_params=pltpu.CompilerParams(
            collective_id=1, has_side_effects=True, vmem_limit_bytes=64000000
        ),
    )(normed, table, hidden, gate, up, down)


def flip(device, bit):
    return device + bit - 2 * bit * ((device // bit) % 2)


def attention_part(
    peers,
    q_ref,
    nope_ref,
    rope_ref,
    value_ref,
    residual_ref,
    segments_ref,
    proj_ref,
    gain_ref,
    hidden_ref,
    normed_ref,
    q_own,
    rope_own,
    stage,
    arrived,
    q_all,
    key_all,
    value_all,
    out_stage,
    attn,
    proj,
    load_sem,
    stage_sem,
    a_send,
    a_recv,
    b_send,
    b_recv,
    c_send,
    c_recv,
):
    block, streams, _ = q_ref.shape
    length = block * peers
    head = NOPE
    width = proj_ref.shape[1]
    proj_rows = proj_ref.shape[0]
    me = lax.axis_index("expert")
    plane = lax.axis_index("dp")
    mate, row_mate = flip(me, 1), flip(me, 2)
    near, far = flip(me, peers // 4), flip(me, peers // 2)

    barrier = pltpu.get_barrier_semaphore()
    for offset in range(1, peers):
        pl.semaphore_signal(
            barrier,
            inc=1,
            device_id={"dp": plane, "expert": (me + offset) % peers},
            device_id_type=MESH,
        )
    pl.semaphore_signal(
        barrier, inc=1, device_id={"dp": 1 - plane, "expert": me}, device_id_type=MESH
    )

    def own_places(device):
        return pl.ds(pl.multiple_of(device * block, block), block)

    def proj_place(part, device):
        return pl.ds(
            pl.multiple_of((part * peers + device) * proj_rows, proj_rows), proj_rows
        )

    load_q = pltpu.make_async_copy(q_ref, q_own, load_sem.at[0])
    load_rope = pltpu.make_async_copy(rope_ref, rope_own, load_sem.at[1])
    load_proj = pltpu.make_async_copy(
        proj_ref, proj.at[proj_place(plane, me)], load_sem.at[2]
    )
    staged = [
        pltpu.make_async_copy(
            src.at[:, :, target * head : (target + 1) * head],
            stage.at[target, 2 + i],
            stage_sem.at[target, i],
        )
        for target in range(peers)
        for i, src in enumerate((nope_ref, value_ref))
    ]
    for load in [load_q, load_rope, load_proj] + staged:
        load.start()
    pl.semaphore_wait(barrier, peers)

    def remote(src, dst, send, recv, part, other):
        return pltpu.make_async_remote_copy(
            src_ref=src,
            dst_ref=dst,
            send_sem=send,
            recv_sem=recv,
            device_id={"dp": part, "expert": other},
            device_id_type=MESH,
        )

    sent = []

    def start(copy):
        copy.start()
        sent.append(copy)

    partners = (
        (plane, far),
        (plane, near),
        (plane, row_mate),
        (1 - plane, me),
        (plane, mate),
    )

    def proj_copy(stage, index, src_part, src_device, from_input=False):
        place = proj.at[proj_place(src_part, src_device)]
        part, other = partners[stage]
        return remote(
            proj_ref if from_input else place,
            place,
            c_send.at[stage, index],
            c_recv.at[stage, index],
            part,
            other,
        )

    def proj_source(index, of_device, of_part):
        device = of_device
        if index & 1:
            device = flip(device, peers // 2)
        if index & 2:
            device = flip(device, peers // 4)
        if index & 4:
            device = flip(device, 2)
        return (1 - of_part if index & 8 else of_part), device

    def proj_forward(index):
        first = index.bit_length()
        part, device = proj_source(index, me, plane)
        for stage in range(first, 5):
            start(proj_copy(stage, index, part, device, from_input=index == 0))

    def proj_wait(index):
        stage = index.bit_length() - 1
        part, device = proj_source(index, me, plane)
        proj_copy(stage, index - (1 << stage), part, device).wait_recv()

    def proj_serve(index):
        proj_wait(index)
        proj_forward(index)

    proj_forward(0)

    def a_copy(offset, source, target):
        return remote(
            stage.at[target],
            arrived.at[source],
            a_send.at[offset],
            a_recv.at[offset],
            plane,
            target if source is me else source,
        )

    order = [(at * 5 + peers // 2) % peers for at in range(peers)]
    order.remove(0)

    load_q.wait()
    load_rope.wait()
    lane = lax.broadcasted_iota(jnp.int32, (block * streams, head), 1)
    low = lane < ROPE

    def wide(x):
        return x.astype(jnp.float32)

    def turn(x):
        return pltpu.roll(x, ROPE, 1)

    rope_once = wide(rope_own[...]).reshape(block * streams, ROPE)
    rope_twice = jnp.concatenate([rope_once, rope_once], axis=1)
    for pair in range(HEADS // 2):
        first = pair * 3 * head
        one, two, three = (
            q_own[:, :, first + i * head : first + (i + 1) * head].reshape(block * streams, head)
            for i in range(3)
        )
        two, three = wide(two), wide(three)
        shape = (block, streams, head)

        def narrow(x):
            return x.astype(jnp.bfloat16).reshape(shape)

        stage[2 * pair, 0] = one.reshape(shape)
        stage[2 * pair, 1] = narrow(jnp.where(low, two, rope_twice))
        stage[2 * pair + 1, 0] = narrow(turn(jnp.where(low, three, two)))
        stage[2 * pair + 1, 1] = narrow(jnp.where(low, rope_twice, three))
    for load in staged:
        load.wait()
    for offset in order[:4]:
        start(a_copy(offset, me, (me + offset) % peers))
    proj_serve(1)
    for offset in order[4:]:
        start(a_copy(offset, me, (me + offset) % peers))

    odd = jnp.full((block, head), me % 2, jnp.int32)
    here = lax.broadcasted_iota(jnp.int32, (block, head), 1) // ROPE
    kept = here == odd

    begins = [
        jnp.sum(1 - segments_ref[stream : stream + 1, :], axis=1, keepdims=True)
        for stream in range(streams)
    ]
    spare = lax.broadcasted_iota(jnp.int32, (block, head), 1) == ROPE * (1 - odd)
    place_in = lax.broadcasted_iota(jnp.int32, (block, head), 0)

    def unpack(blocks, device):
        places = own_places(device)
        for stream in range(streams):
            second = place_in + device * block >= begins[stream]
            q_mark = jnp.where(spare & second, 1.0, 0.0)
            key_mark = jnp.where(spare & jnp.logical_not(second), FAR_BELOW, 0.0)
            mix = wide(blocks[device, 1, :, stream, :])
            q_all[stream, places, :head] = blocks[device, 0, :, stream, :]
            q_all[stream, places, head:] = jnp.where(kept, mix, q_mark).astype(jnp.bfloat16)
            key_all[stream, places, :head] = blocks[device, 2, :, stream, :]
            key_all[stream, places, head:] = jnp.where(kept, turn(mix), key_mark).astype(
                jnp.bfloat16
            )
            value_all[stream, places, :] = blocks[device, 3, :, stream, :]

    unpack(stage, me)
    proj_serve(2)
    proj_serve(3)
    served = 4
    for offset in order:
        source = (me + peers - offset) % peers
        a_copy(offset, source, me).wait_recv()
        unpack(arrived, source)
        if served < 12:
            proj_serve(served)
            served += 1

    scale = (NOPE + ROPE) ** (-0.5) * 1.4426950408889634
    query_rows = length // 4
    group = query_rows // block
    spot_row = lax.broadcasted_iota(jnp.int32, (block * streams, block * streams), 0)
    spot_column = lax.broadcasted_iota(jnp.int32, (block * streams, block * streams), 1)
    weave = jnp.where(
        spot_column == (spot_row % streams) * block + spot_row // streams, 1.0, 0.0
    ).astype(jnp.bfloat16)

    def b_copy(target):
        return remote(
            out_stage.at[target],
            attn.at[me],
            b_send.at[target],
            b_recv.at[me],
            plane,
            target,
        )

    causal = lax.broadcasted_iota(jnp.int32, (query_rows, query_rows), 1) <= (
        lax.broadcasted_iota(jnp.int32, (query_rows, query_rows), 0)
    )
    for part in (3, 0, 2, 1):
        rows = pl.ds(part * query_rows, query_rows)
        seen = (part + 1) * query_rows
        outs = []
        for stream in range(streams):
            scores = lax.dot_general(
                q_all[stream, rows, :],
                key_all[stream, :seen, :],
                (((1,), (1,)), ((), ())),
                preferred_element_type=jnp.float32,
            )
            corner = jnp.where(causal, scores[:, seen - query_rows :], -jnp.inf)
            if part:
                scores = jnp.concatenate([scores[:, : seen - query_rows], corner], axis=1)
            else:
                scores = corner
            peak = jnp.max(scores, axis=1, keepdims=True)
            raised = jnp.exp2((scores - peak) * scale)
            total = jnp.sum(raised, axis=1, keepdims=True)
            mixed = jnp.dot(
                raised.astype(jnp.bfloat16),
                value_all[stream, :seen, :],
                preferred_element_type=jnp.float32,
            )
            outs.append((mixed / total).astype(jnp.bfloat16))
        for at in range(group):
            target = part * group + at
            both = jnp.concatenate(
                [out[at * block : (at + 1) * block, :] for out in outs], axis=0
            )
            out_stage[target] = jnp.dot(
                weave, both, preferred_element_type=jnp.float32
            ).astype(jnp.bfloat16)

            @pl.when(me != target)
            def _():
                b_copy(target).start()

            @pl.when(me == target)
            def _():
                attn[target] = out_stage[target]

    while served < 16:
        proj_wait(served)
        start(
            proj_copy(4, served, *proj_source(served, me, plane))
        )
        served += 1
    load_proj.wait()
    for index in range(16):
        part, device = proj_source(index, mate, plane)
        proj_copy(4, index, part, device).wait_recv()

    for offset in order:
        source = (me + peers - offset) % peers
        remote(
            out_stage.at[source],
            attn.at[source],
            b_send.at[source],
            b_recv.at[source],
            plane,
            source,
        ).wait_recv()
    mixed_rows = jnp.concatenate([attn[at] for at in range(peers)], axis=1)
    squares = jnp.zeros((block * streams, 1), jnp.float32)
    step = 4 * head
    for first in range(0, width, step):
        projected = jnp.dot(
            mixed_rows, proj[:, first : first + step], preferred_element_type=jnp.float32
        )
        before = jnp.concatenate(
            [
                residual_ref[:, :, at : at + head].reshape(block * streams, head)
                for at in range(first, first + step, head)
            ],
            axis=1,
        )
        hidden = before.astype(jnp.float32) + projected
        hidden_ref[:, first : first + step] = hidden
        squares = squares + jnp.sum(hidden * hidden, axis=1, keepdims=True)
    factor = lax.rsqrt(squares * (1.0 / width) + EPSILON)
    for first in range(0, width, step):
        gain = gain_ref[first : first + step].astype(jnp.float32).reshape(1, step)
        normed_ref[:, first : first + step] = (
            hidden_ref[:, first : first + step] * factor * gain
        ).astype(jnp.bfloat16)

    yield
    for copy in sent:
        copy.wait_send()
    for target in range(peers):

        @pl.when(me != target)
        def _():
            b_copy(target).wait_send()
    yield


def layer_kernel(
    peers,
    q_ref,
    nope_ref,
    rope_ref,
    value_ref,
    residual_ref,
    segments_ref,
    proj_ref,
    gain_ref,
    routes_ref,
    weights_ref,
    gate_ref,
    up_ref,
    down_ref,
    out_ref,
    hidden,
    normed,
    table,
    *scratch,
):
    block, streams, width = out_ref.shape
    split = 18
    attention = attention_part(
        peers,
        q_ref,
        nope_ref,
        rope_ref,
        value_ref,
        residual_ref,
        segments_ref,
        proj_ref,
        gain_ref,
        hidden,
        normed,
        *scratch[:split],
    )

    def store(first, rows):
        count = rows.shape[0] // streams
        for at in range(0, width, NOPE):
            out_ref[pl.ds(first // streams, count), :, at : at + NOPE] = rows[
                :, at : at + NOPE
            ].reshape(count, streams, NOPE)

    experts = expert_part(
        peers // 2,
        False,
        store,
        normed,
        table,
        hidden,
        gate_ref,
        up_ref,
        down_ref,
        *scratch[split:],
    )
    choices, tokens = routes_ref.shape[0], routes_ref.shape[2]
    ids = lax.broadcasted_iota(jnp.int32, (peers, tokens), 0)
    sums = jnp.zeros((peers, tokens), jnp.float32)
    for at in range(choices):
        sums = sums + jnp.where(ids == routes_ref[at], weights_ref[at], 0.0)
    table[...] = sums
    next(experts)
    next(attention)
    next(experts)
    next(attention)


def whole_layer(
    queries,
    key_nope,
    key_rope,
    values,
    residual,
    segments,
    out_proj,
    norm_gain,
    routes,
    route_weights,
    gate,
    up,
    down,
    peers,
):
    block, streams, q_width = queries.shape
    width = residual.shape[2]
    tokens = block * streams
    length = block * peers
    vmem = pl.BlockSpec(memory_space=pltpu.VMEM)
    anywhere = pl.BlockSpec(memory_space=pl.ANY)
    dma = pltpu.SemaphoreType.DMA
    blocks = pltpu.VMEM((peers, 4, block, streams, NOPE), jnp.bfloat16)
    attention_scratch = [
        pltpu.VMEM((block, streams, q_width), jnp.bfloat16),
        pltpu.VMEM((block, streams, ROPE), jnp.bfloat16),
        blocks,
        blocks,
        pltpu.VMEM((streams, length, 2 * NOPE), jnp.bfloat16),
        pltpu.VMEM((streams, length, 2 * NOPE), jnp.bfloat16),
        pltpu.VMEM((streams, length, V_DIM), jnp.bfloat16),
        pltpu.VMEM((peers, tokens, V_DIM), jnp.bfloat16),
        pltpu.VMEM((peers, tokens, V_DIM), jnp.bfloat16),
        pltpu.VMEM((HEADS * V_DIM, width), jnp.bfloat16),
        dma((3,)),
        dma((peers, 2)),
        dma((peers,)),
        dma((peers,)),
        dma((peers,)),
        dma((peers,)),
        dma((5, 16)),
        dma((5, 16)),
    ]
    layer_out = pl.pallas_call(
        functools.partial(layer_kernel, peers),
        out_shape=jax.ShapeDtypeStruct((block, streams, width), jnp.bfloat16),
        in_specs=[anywhere] * 4 + [vmem, vmem, anywhere, vmem, vmem, vmem] + [anywhere] * 3,
        out_specs=vmem,
        scratch_shapes=[
            pltpu.VMEM((tokens, width), jnp.float32),
            pltpu.VMEM((tokens, width), jnp.bfloat16),
            pltpu.VMEM((peers, tokens), jnp.float32),
        ]
        + attention_scratch
        + expert_scratch(tokens, width, peers, gate.shape[0]),
        compiler_params=pltpu.CompilerParams(
            collective_id=0, has_side_effects=True, vmem_limit_bytes=64000000
        ),
    )(
        queries,
        key_nope,
        key_rope,
        values,
        residual,
        segments,
        out_proj,
        norm_gain,
        jnp.transpose(routes, (3, 0, 1, 2)).reshape(-1, 1, tokens),
        jnp.transpose(route_weights, (3, 0, 1, 2)).reshape(-1, 1, tokens),
        gate,
        up,
        down,
    )
    return pl.pallas_call(
        copy_kernel,
        out_shape=jax.ShapeDtypeStruct(layer_out.shape, layer_out.dtype),
        in_specs=[vmem],
        out_specs=anywhere,
        scratch_shapes=[dma],
    )(layer_out)


def copy_kernel(x_ref, out_ref, sem):
    copy = pltpu.make_async_copy(x_ref, out_ref, sem)
    copy.start()
    copy.wait()


def attend_items(query_items, key_items, value_items, segment_items):
    length, count_items, qk_width = query_items.shape
    block_rows = QUERY_BLOCK
    score_scale = qk_width ** (-0.5)
    key_positions = jnp.arange(length, dtype=jnp.int32)

    def one_block(block_index):
        first_row = block_index * block_rows
        query_block = lax.dynamic_slice_in_dim(query_items, first_row, block_rows, 0)
        scores = (
            jnp.einsum("qid,kid->iqk", query_block, key_items, preferred_element_type=jnp.float32)
            * score_scale
        )
        row_positions = first_row + jnp.arange(block_rows, dtype=jnp.int32)
        row_segments = lax.dynamic_slice_in_dim(segment_items, first_row, block_rows, 1)
        allowed = (row_positions[None, :, None] >= key_positions[None, None, :]) & (
            row_segments[:, :, None] == segment_items[:, None, :]
        )
        scores = jnp.where(allowed, scores, -jnp.inf)
        row_peak = jnp.max(scores, axis=2, keepdims=True)
        raised = jnp.exp(scores - row_peak)
        weights = (raised / jnp.sum(raised, axis=2, keepdims=True)).astype(jnp.bfloat16)
        return jnp.einsum(
            "iqk,kid->qid", weights, value_items, preferred_element_type=jnp.float32
        ).astype(jnp.bfloat16)

    blocks = lax.map(one_block, jnp.arange(length // block_rows, dtype=jnp.int32))
    return blocks.reshape(length, count_items, value_items.shape[2])


def attend_by_heads(
    queries, key_nope, key_rope, values, residual, segments, out_proj, norm_gain, expert_count
):
    half_rows, stream_count, query_width = queries.shape
    model_width = residual.shape[2]
    token_rows = half_rows * stream_count
    item_count = stream_count * HEADS // expert_count
    key_heads = jnp.concatenate(
        [
            key_nope.reshape(half_rows, stream_count, HEADS, NOPE),
            jnp.broadcast_to(key_rope[:, :, None, :], (half_rows, stream_count, HEADS, ROPE)),
        ],
        axis=3,
    )
    query_items = queries.reshape(half_rows, stream_count * HEADS, NOPE + ROPE)
    key_items = key_heads.reshape(half_rows, stream_count * HEADS, NOPE + ROPE)
    value_items = values.reshape(half_rows, stream_count * HEADS, V_DIM)
    packed = jnp.concatenate([query_items, key_items, value_items], axis=2)
    packed_all = lax.all_to_all(packed, "expert", split_axis=1, concat_axis=0, tiled=True)
    qk_width = NOPE + ROPE
    query_all = packed_all[:, :, :qk_width]
    key_all = packed_all[:, :, qk_width : 2 * qk_width]
    value_all = packed_all[:, :, 2 * qk_width :]
    item_ids = lax.axis_index("expert") * item_count + jnp.arange(item_count, dtype=jnp.int32)
    stream_ids = item_ids // HEADS
    selector = (stream_ids[:, None] == jnp.arange(stream_count, dtype=jnp.int32)[None, :]).astype(
        jnp.int32
    )
    segment_items = jnp.sum(selector[:, :, None] * segments[None, :, :], axis=1)
    attended_items = attend_items(query_all, key_all, value_all, segment_items)
    attended_back = lax.all_to_all(
        attended_items, "expert", split_axis=0, concat_axis=1, tiled=True
    )
    attn_rows = attended_back.reshape(token_rows, HEADS * V_DIM)
    projected = jnp.dot(
        attn_rows,
        lax.all_gather(out_proj, ("dp", "expert"), axis=0, tiled=True),
        preferred_element_type=jnp.float32,
    )
    hidden = residual.reshape(token_rows, model_width).astype(jnp.float32) + projected
    mean_square = jnp.mean(hidden * hidden, axis=1, keepdims=True)
    normed = (hidden * lax.rsqrt(mean_square + EPSILON) * norm_gain.astype(jnp.float32)).astype(
        jnp.bfloat16
    )
    return hidden, normed


def body(
    queries,
    key_nope,
    key_rope,
    values,
    residual,
    segments,
    out_proj,
    norm_gain,
    expert_gate,
    expert_up,
    expert_down,
    routes,
    route_weights,
):
    half_rows, stream_count, query_width = queries.shape
    model_width = residual.shape[2]
    token_rows = half_rows * stream_count
    expert_count = lax.axis_size("expert")
    gate = jnp.swapaxes(expert_gate[0], 0, 1)
    up = jnp.swapaxes(expert_up[0], 0, 1)
    attention_inputs = (
        queries,
        key_nope,
        key_rope,
        values,
        residual,
        segments,
        out_proj,
        norm_gain,
    )
    if expert_count == HEADS and lax.axis_size("dp") == 2 and stream_count == 2:
        return whole_layer(
            *attention_inputs, routes, route_weights, gate, up, expert_down[0], expert_count
        )
    hidden, normed = attend_by_heads(*attention_inputs, expert_count)
    token_routes = routes.reshape(token_rows, TOP)
    token_weights = route_weights.reshape(token_rows, TOP)
    expert_ids = jnp.arange(expert_count, dtype=jnp.int32)
    weight_table = jnp.sum(
        jnp.where(
            token_routes[:, :, None] == expert_ids[None, None, :], token_weights[:, :, None], 0.0
        ),
        axis=1,
    )
    layer_out = routed_experts(
        normed, weight_table.T, hidden, gate, up, expert_down[0]
    )
    return layer_out.reshape(half_rows, stream_count, model_width)


def solution(mesh):
    return jax.shard_map(
        body,
        mesh=mesh,
        in_specs=(
            P("expert", "dp", None),
            P("expert", "dp", None),
            P("expert", "dp", None),
            P("expert", "dp", None),
            P("expert", "dp", None),
            P("dp", None),
            P(("dp", "expert"), None),
            P(),
            P("expert", None, None),
            P("expert", None, None),
            P("expert", None, None),
            P("dp", "expert", None, None),
            P("dp", "expert", None, None),
        ),
        out_specs=P("expert", "dp", None),
        check_vma=False,
    )
```
